128 devices in a mesh: seq: 8 (over x_lo, z), tp: 8 (over y, core), roll: 2 (over x_hi).
Axes of the slice: x: 4 (x_hi: 2, x_lo: 2; x = x_hi * 2 + x_lo), y: 4, z: 4, core: 2. Of those that a mesh axis runs over, the one named last changes fastest.
Arguments:
- hidden: bfloat16 [8, 3584], P('roll'), may hold values from -6 to 6
- norm_gain: bfloat16 [3584], replicated, may hold values from 0.25 to 1.75
- qkv_bias: bfloat16 [3072], replicated, may hold values from -20 to 20
- qkv_weight: bfloat16 [3584, 3072], P(('seq', 'tp', 'roll')), may hold values from -0.09375 to 0.09375
- out_weight: bfloat16 [3584, 2048], P(('seq', 'tp', 'roll')), may hold values from -0.125 to 0.125
- key_cache: bfloat16 [8, 65536, 512], P('roll', ('seq', 'tp')), may hold values from -16 to 16
- value_cache: bfloat16 [8, 65536, 512], P('roll', ('seq', 'tp')), may hold values from -16 to 16
- cache_len: int32 [8], P('roll'), may hold values from 32768 to 65536, as said below
- block_pos: int32 [8, 128], P('roll', ('seq', 'tp')), may hold values from 0 to 16383, as said below
Outputs:
- attended: bfloat16 [8, 3584], P('roll')
- fresh_kv: bfloat16 [8, 1024], P('roll')
- served_qkv: bfloat16 [3584, 4096], P(None, 'tp')
- served_out: bfloat16 [3584, 2048], P(None, 'tp')
The draws below stay inside these ranges and needn't reach their ends.
Inputs may be any that keep to these rules, and one draw needn't show every extreme that they name: `cache_len`: in every draw one rollout has all 65536 positions cached. With i = cache_len[r] mod 8192, and c the 8192-position stretch that holds position cache_len[r]: block_pos[r, b] is i where block b lies in c, i + 8192 where it lies in a later stretch or in the stretch just before c, and 16383 elsewhere.
All inputs are finite; a program needn't handle non-finite values.
Results may differ from the reference program's by a relative error of at most 0.009.
Values may be sent and summed in bfloat16 or wider, within the bound.
A program may use at most 128 MiB of HBM per device.

```python
import jax
import jax.numpy as jnp
import numpy as np
from jax import lax

D = 3584
HQ = 16
KVH = 4
HD = 128
QKV = 3072
SCOLS = 512
ROLLS = 8
LEN = 65536
BLOCK = 512
NBLK = 128
STRETCH = 8192
N_TP = 8


def shared_lengths(key):
    base_draw = jax.random.randint(jax.random.fold_in(key, 11), (ROLLS,), LEN // 2, LEN + 1)
    chosen = jax.random.randint(jax.random.fold_in(key, 12), (), 0, ROLLS)
    return jnp.where(jnp.arange(ROLLS) == chosen, LEN, base_draw).astype(jnp.int32)


def draw_cache_len(key, part):
    return shared_lengths(key)


def draw_block_pos(key, part):
    lengths = shared_lengths(key)
    block_stretch = jnp.arange(NBLK, dtype=jnp.int32) * BLOCK // STRETCH
    query_stretch = (lengths // STRETCH)[:, None]
    intra_pos = (lengths % STRETCH)[:, None]
    near_pos = jnp.where(block_stretch[None, :] == query_stretch, intra_pos, intra_pos + STRETCH)
    return jnp.where(block_stretch[None, :] >= query_stretch - 1, near_pos, 2 * STRETCH - 1).astype(jnp.int32)


def draw_qkv_bias(key, part):
    bias_draw = 0.5 * jax.random.normal(jax.random.fold_in(key, 31), (QKV,), jnp.float32)
    return jnp.clip(bias_draw, -20.0, 20.0).astype(jnp.bfloat16)


def draw_key_cache(key, part):
    col_total = KVH * HD
    noise_part = jax.random.normal(jax.random.fold_in(key, 41), (ROLLS, NBLK, BLOCK, col_total), jnp.float32)
    region_mean = jax.random.normal(jax.random.fold_in(key, 42), (ROLLS, NBLK, 1, col_total), jnp.float32)
    cached = (noise_part + 0.5 * region_mean).reshape(ROLLS, LEN, col_total)
    return jnp.clip(cached, -16.0, 16.0).astype(jnp.bfloat16)


def draw_value_cache(key, part):
    col_total = KVH * HD
    region_mean = jax.random.normal(jax.random.fold_in(key, 52), (ROLLS, NBLK, 1, col_total), jnp.float32)
    noise_part = jax.random.normal(jax.random.fold_in(key, 51), (ROLLS, NBLK, BLOCK, col_total), jnp.float32)
    cached = noise_part + 2.0 * region_mean
    return jnp.clip(cached.reshape(ROLLS, LEN, col_total), -16.0, 16.0).astype(jnp.bfloat16)


def level_of(key, extent, cuts, smallest, largest):
    gain, own = 1.0, jax.random.fold_in(key, 6)
    for dim, shards_of in cuts:
        steps = jnp.exp(jax.random.uniform(jax.random.fold_in(own, dim), (shards_of,), jnp.float32, smallest / len(cuts), largest / len(cuts)))
        gain = gain * jnp.repeat(steps, extent[dim] // shards_of).reshape([-1 if axis == dim else 1 for axis in range(len(extent))])
    return gain


def centred(rng, dims, deviation, bound, pieces=(), kind=jnp.bfloat16):
    values = jax.random.normal(rng, dims, jnp.float32) * deviation
    if len(pieces) > 0:
        values = level_of(rng, dims, pieces, -0.22, 0.18) * values
    return jnp.clip(values, min=-bound, max=bound).astype(kind)


def setup_inputs(seed: int = 0) -> dict:
    keys = jax.random.split(jax.random.key(seed), 10)
    return {
        "hidden": centred(keys[0], (ROLLS, D), 1.0, 6.0, ((0, 2),)),
        "norm_gain": jnp.clip(1.0 + 0.15 * jax.random.normal(keys[1], (D,), jnp.float32), 0.25, 1.75).astype(jnp.bfloat16),
        "qkv_bias": draw_qkv_bias(jax.random.fold_in(keys[9], 71), 0),
        "qkv_weight": centred(keys[3], (D, QKV), D ** -0.5, 0.09375, ((0, 128),)),
        "out_weight": centred(keys[4], (D, HQ * HD), (HQ * HD) ** -0.5, 0.125, ((0, 128),)),
        "key_cache": draw_key_cache(jax.random.fold_in(keys[9], 71), 0),
        "value_cache": draw_value_cache(jax.random.fold_in(keys[9], 71), 0),
        "cache_len": draw_cache_len(jax.random.fold_in(keys[9], 71), 0),
        "block_pos": draw_block_pos(jax.random.fold_in(keys[9], 71), 0),
    }


rope_base = 10000000.0
norm_eps = 1e-06

def frequencies(width):
    half_width = width // 2
    exact = rope_base ** (-2.0 * np.arange(half_width) / width)
    octave = np.floor(np.log2(exact))
    quantum = 2.0 ** (8.0 - octave)
    return np.floor(exact * quantum) / quantum

def rotate(vectors, positions):
    half_width = vectors.shape[-1] // 2
    inverse = jnp.asarray(frequencies(vectors.shape[-1]), dtype=jnp.float32)
    angles = positions.astype(jnp.float32)[..., None] * inverse
    cosine = jnp.cos(angles)
    sine_part = jnp.sin(angles)
    front_half = vectors[..., :half_width]
    back_half = vectors[..., half_width:]
    return jnp.concatenate([front_half * cosine - back_half * sine_part, back_half * cosine + front_half * sine_part], axis=-1)

def arrange(columns, tp_count):
    lead = columns.shape[:-1]
    per_rank = HQ // tp_count
    query_part = columns[..., :HQ * HD].reshape(lead + (tp_count, per_rank * HD))
    key_part = jnp.repeat(columns[..., HQ * HD:(HQ + KVH) * HD].reshape(lead + (KVH, HD)), tp_count // KVH, axis=-2)
    value_part = jnp.repeat(columns[..., (HQ + KVH) * HD:].reshape(lead + (KVH, HD)), tp_count // KVH, axis=-2)
    return jnp.concatenate([query_part, key_part, value_part], axis=-1)

def reference(hidden, norm_gain, qkv_bias, qkv_weight, out_weight, key_cache, value_cache, cache_len, block_pos):
    group_size = HQ // KVH
    score_scale = HD ** (-0.5)
    hidden_wide = hidden.astype(jnp.float32)
    normed = (hidden_wide * lax.rsqrt(lax.optimization_barrier(jnp.mean(hidden_wide * hidden_wide, axis=1, keepdims=True)) + norm_eps) * norm_gain.astype(jnp.float32)).astype(jnp.bfloat16)
    joint = (jnp.dot(normed, qkv_weight, preferred_element_type=jnp.float32) + qkv_bias.astype(jnp.float32)).astype(jnp.bfloat16)
    queries = joint[:, :HQ * HD].reshape(ROLLS, HQ, HD).astype(jnp.float32)
    new_keys = joint[:, HQ * HD:(HQ + KVH) * HD].reshape(ROLLS, KVH, HD).astype(jnp.float32)
    fresh_value = joint[:, (HQ + KVH) * HD:].reshape(ROLLS, KVH, HD)
    intra_pos = (cache_len % STRETCH).astype(jnp.int32)
    fresh_key = lax.optimization_barrier(rotate(new_keys, jnp.broadcast_to(intra_pos[:, None], (ROLLS, KVH))).astype(jnp.bfloat16))
    self_query = lax.optimization_barrier(rotate(queries, jnp.broadcast_to(intra_pos[:, None], (ROLLS, HQ))).astype(jnp.bfloat16))
    block_query = lax.optimization_barrier(rotate(queries[:, None], jnp.broadcast_to(block_pos[:, :, None], (ROLLS, NBLK, HQ))).astype(jnp.bfloat16))
    self_score = score_scale * jnp.einsum('rkgd,rkd->rkg', self_query.reshape(ROLLS, KVH, group_size, HD).astype(jnp.float32), fresh_key.astype(jnp.float32))

    def one_rollout(per_rollout):
        cached_keys, cached_values, rotated_query, length, own_score, own_value = per_rollout
        keys_wide = cached_keys.reshape(NBLK, BLOCK, KVH, HD).astype(jnp.float32)
        values_wide = cached_values.reshape(NBLK, BLOCK, KVH, HD).astype(jnp.float32)
        query_wide = rotated_query.reshape(NBLK, KVH, group_size, HD).astype(jnp.float32)
        scores = score_scale * jnp.einsum('bkgd,bpkd->kgbp', query_wide, keys_wide)
        valid_mask = jnp.arange(LEN, dtype=jnp.int32).reshape(NBLK, BLOCK) < length
        masked = jnp.where(valid_mask, scores, -jnp.inf)
        top_score = jnp.maximum(lax.optimization_barrier(jnp.max(masked, axis=(2, 3))), own_score)
        weights = jnp.where(valid_mask, jnp.exp(masked - top_score[:, :, None, None]), 0.0)
        own_weight = jnp.exp(own_score - top_score)
        rounded = lax.optimization_barrier(weights.astype(jnp.bfloat16)).astype(jnp.float32)
        own_rounded = lax.optimization_barrier(own_weight.astype(jnp.bfloat16)).astype(jnp.float32)
        numerator = jnp.einsum('kgbp,bpkd->kgd', rounded, values_wide) + own_rounded[:, :, None] * own_value.astype(jnp.float32)[:, None, :]
        denominator = lax.optimization_barrier(jnp.sum(weights, axis=(2, 3))) + own_weight
        return (numerator / denominator[:, :, None]).reshape(HQ * HD).astype(jnp.bfloat16)
    attention = lax.map(one_rollout, (key_cache, value_cache, block_query, cache_len, self_score, fresh_value))
    attended = jnp.dot(attention, out_weight.T, preferred_element_type=jnp.float32).astype(jnp.bfloat16)
    fresh_kv = jnp.concatenate([fresh_key.reshape(ROLLS, KVH * HD), fresh_value.reshape(ROLLS, KVH * HD)], axis=1)
    served_qkv = arrange(qkv_weight, N_TP).reshape(D, N_TP * SCOLS)
    return (attended, fresh_kv, served_qkv, out_weight)
```

```python
import jax
import jax.numpy as jnp
import numpy as np
from jax import lax
from jax.experimental import pallas as pl
from jax.experimental.pallas import tpu as pltpu
from jax.sharding import Mesh
from jax.sharding import PartitionSpec as P

HQ = 16
KVH = 4
HD = 128
BLOCK = 512
STRETCH = 8192
TP = ("tp_0", "tp_1")
SEQ = ("seq_0", "seq_1")
SEQ_TP = ("seq_0", "seq_1", "tp_0", "tp_1")
SEQ_TP_ROLL = ("seq_0", "seq_1", "tp_0", "tp_1", "roll")


rope_base = 10000000.0
norm_eps = 1e-06
floor_score = -1e30


MESH = pl.DeviceIdType.MESH
WAVES = (0, 1, 3, 2)
GROUPS = 7


def place():
    x = lax.axis_index("roll") * 2 + lax.axis_index("seq_0")
    return x, lax.axis_index("tp_0"), lax.axis_index("seq_1"), lax.axis_index("tp_1")


def device(x, y, z, core):
    return (x % 2, z, y, core, x // 2)


def relay_kernel(src_ref, w_ref, own_sem, trade_send, trade_recv, ring_send, ring_recv):
    x, y, z, core = place()

    def remote(src, dst, send, recv, target):
        return pltpu.make_async_remote_copy(
            src_ref=src, dst_ref=dst, send_sem=send, recv_sem=recv,
            device_id=device(*target), device_id_type=MESH,
        )

    def slot(bx, bz, tiles, first, count):
        return w_ref.at[pl.ds(*tiles), (bx % 2) * 4 + bz, pl.ds(first, count), bx // 2]

    barrier = pltpu.get_barrier_semaphore()
    partners = [(x, (y + dy) % 4, z, (core + dc) % 2) for dy in range(4) for dc in range(2) if dy + dc > 0]
    partners += [((x + d) % 4, y, z, core) for d in (1, 3)]
    partners += [(x, y, (z + d) % 4, core) for d in (1, 3)]
    for partner in partners:
        pl.semaphore_signal(barrier, inc=1, device_id=device(*partner), device_id_type=MESH)
    pl.semaphore_wait(barrier, len(partners))

    def traded(dy, dc):
        there = ((y + dy) % 4, (core + dc) % 2)
        return remote(
            src_ref.at[there[0] * 2 + there[1]],
            w_ref.at[:, (x % 2) * 4 + z, y * 2 + core, x // 2],
            trade_send.at[dy * 2 + dc], trade_recv.at[dy * 2 + dc],
            (x, there[0], z, there[1]),
        )

    def arrived(dy, dc):
        from_tp = ((y - dy) % 4) * 2 + (core + dc) % 2
        here = w_ref.at[:, (x % 2) * 4 + z, from_tp, x // 2]
        return remote(here, here, trade_send.at[dy * 2 + dc], trade_recv.at[dy * 2 + dc],
                      (x, (y + dy) % 4, z, (core + dc) % 2))

    own = pltpu.make_async_copy(
        src_ref.at[y * 2 + core], w_ref.at[:, (x % 2) * 4 + z, y * 2 + core, x // 2], own_sem
    )
    traded(0, 1).start()
    own.start()
    for dy in (3, 1, 2):
        for dc in (0, 1):
            traded(dy, dc).start()

    def ring(wave, half, kind, f, g, part, step):
        first = ((y + WAVES[wave]) % 4) * 2
        tiles = (half * 3, 3)
        df, dg = step
        if half == 0:
            bx, bz, tx, tz = x + g, z + f, x + dg, z + df
        else:
            bx, bz, tx, tz = x + f, z + g, x + df, z + dg
        bx, bz, tx, tz = bx % 4, bz % 4, tx % 4, tz % 4
        block = slot(bx, bz, tiles, first + (0 if part is None else part), 2 if part is None else 1)
        return remote(block, block, ring_send.at[wave], ring_recv.at[wave, half * 20 + kind], (tx, y, tz, core))

    order = (0, -1, 1, 2)

    def sideways(wave, half, f):
        k = 4 + order.index(f) * 4
        ring(wave, half, k, f, 0, None, (0, 1)).start()
        ring(wave, half, k + 1, f, 0, None, (0, -1)).start()

    def s1(wave):
        if wave == 0:
            own.wait()
            arrived(0, 1).wait_recv()
        else:
            dy = (-WAVES[wave]) % 4
            arrived(dy, 0).wait_recv()
            arrived(dy, 1).wait_recv()
        for half in (0, 1):
            ring(wave, half, 0, 0, 0, None, (1, 0)).start()
            ring(wave, half, 1, 0, 0, None, (-1, 0)).start()
        for half in (0, 1):
            sideways(wave, half, 0)

    def s2(wave):
        for half in (0, 1):
            ring(wave, half, 0, -1, 0, None, (1, 0)).wait_recv()
            ring(wave, half, 2, -1, 0, 0, (1, 0)).start()
            ring(wave, half, 1, 1, 0, None, (1, 0)).wait_recv()
            ring(wave, half, 3, 1, 0, 1, (-1, 0)).start()
        for half in (0, 1):
            sideways(wave, half, -1)
            sideways(wave, half, 1)

    def s3(wave):
        for half in (0, 1):
            ring(wave, half, 2, 2, 0, 0, (1, 0)).wait_recv()
            ring(wave, half, 3, 2, 0, 1, (1, 0)).wait_recv()
            sideways(wave, half, 2)

    def s4(wave):
        for f in order:
            for half in (0, 1):
                k = 4 + order.index(f) * 4
                ring(wave, half, k, f, -1, None, (0, 1)).wait_recv()
                ring(wave, half, k + 2, f, -1, 0, (0, 1)).start()
                ring(wave, half, k + 1, f, 1, None, (0, 1)).wait_recv()
                ring(wave, half, k + 3, f, 1, 1, (0, -1)).start()

    def s5(wave):
        for f in order:
            for half in (0, 1):
                k = 4 + order.index(f) * 4
                ring(wave, half, k + 2, f, 2, 0, (0, 1)).wait_recv()
                ring(wave, half, k + 3, f, 2, 1, (0, 1)).wait_recv()
        sent = w_ref.at[:, 0:5, 0:6, 0]
        remote(sent, sent, ring_send.at[wave], ring_recv.at[wave, 0], (x, y, (z + 1) % 4, core)).wait_send()

    for step, wave in ((s1, 0), (s1, 1), (s2, 0), (s3, 0), (s1, 2), (s2, 1), (s4, 0), (s3, 1), (s1, 3),
                       (s2, 2), (s4, 1), (s3, 2), (s2, 3), (s4, 2), (s3, 3), (s4, 3)):
        step(wave)
    for wave in range(4):
        s5(wave)
    for dy in range(4):
        for dc in (0, 1):
            if dy + dc > 0:
                traded(dy, dc).wait_send()


def relay(src):
    return pl.pallas_call(
        relay_kernel,
        name="relay",
        out_shape=jax.ShapeDtypeStruct((6, 8, 8, 2, GROUPS, 4, HD), jnp.bfloat16),
        in_specs=[pl.BlockSpec(memory_space=pltpu.HBM)],
        out_specs=pl.BlockSpec(memory_space=pltpu.VMEM),
        scratch_shapes=[
            pltpu.SemaphoreType.DMA,
            pltpu.SemaphoreType.DMA((8,)),
            pltpu.SemaphoreType.DMA((8,)),
            pltpu.SemaphoreType.DMA((4,)),
            pltpu.SemaphoreType.DMA((4, 40)),
        ],
        compiler_params=pltpu.CompilerParams(collective_id=0, has_side_effects=True, vmem_limit_bytes=30 * 2**20),
    )(src)


def from_everyone(array, axis):
    copies = jnp.broadcast_to(array, (lax.axis_size(axis), *array.shape))
    return lax.all_to_all(copies, axis, split_axis=0, concat_axis=0, tiled=True)


def joined_along(parts, dim):
    dims = list(parts.shape[1:])
    dims[dim] *= parts.shape[0]
    return jnp.moveaxis(parts, 0, dim).reshape(dims)


def gather_directly(array, axis, dim):
    parts = from_everyone(array, axis)
    return joined_along(parts, dim)


def side_by_side(arrays, axis, dim, along):
    both = jnp.concatenate(arrays, axis=along)
    whole, at, outs = (gather_directly(both, axis, dim), 0, [])
    for a in arrays:
        outs.append(lax.slice_in_dim(whole, at, at + a.shape[along], axis=along))
        at += a.shape[along]
    return tuple(outs)


def side_by_side_2(arrays, axis, split_dim, concat_dim, along):
    widths = [a.shape[along] for a in arrays]
    both = jnp.concatenate(arrays, axis=along)
    whole = lax.all_to_all(both, axis, split_axis=split_dim, concat_axis=concat_dim, tiled=True)
    return tuple(jnp.split(whole, [sum(widths[:k]) for k in range(1, len(widths))], axis=along))


def side_by_side_3(arrays, axis, dim, along):
    both = jnp.concatenate(arrays, axis=along)
    whole, at, outs = (lax.all_gather(both, axis, axis=dim, tiled=True), 0, [])
    for a in arrays:
        outs.append(lax.slice_in_dim(whole, at, at + a.shape[along], axis=along))
        at += a.shape[along]
    return tuple(outs)


def gathered_once(array, axis):
    leaves = jax.tree.leaves(array)
    turns = sorted(range(len(leaves)), key=lambda k: -leaves[k].size)
    width = (1, *leaves[turns[0]].shape)[-1]
    lines = [
        jnp.pad(leaves[k].reshape(-1), (0, -leaves[k].size % width)).reshape(-1, width)
        for k in turns
    ]
    both, at, found = (lax.all_gather(jnp.concatenate(lines), axis), 0, {})
    for k, line in zip(turns, lines):
        piece = both[:, at : at + len(line)].reshape(len(both), -1)
        found[k] = piece[:, : leaves[k].size].reshape(-1, *leaves[k].shape)
        at += len(line)
    numbers = iter(range(len(leaves)))
    return jax.tree.map(lambda _: found[next(numbers)], array)


def combined_by_axis(array, axes, combine):
    for axis in axes:
        pieces = gathered_once(array, axis)
        array = jax.tree.map(lambda part: part[0], pieces)
        for k in range(1, lax.axis_size(axis)):
            array = combine(array, jax.tree.map(lambda part: part[k], pieces))
    return array


def of_everyone(array, axis):
    everything = from_everyone(array, axis)
    return jnp.sum(everything, axis=0)


def frequencies(width):
    half_width = width // 2
    exact = rope_base ** (-2.0 * np.arange(half_width) / width)
    octave = np.floor(np.log2(exact))
    quantum = 2.0 ** (8.0 - octave)
    return np.floor(exact * quantum) / quantum


def rotate(vectors, positions):
    half_width = vectors.shape[-1] // 2
    inverse = jnp.asarray(frequencies(vectors.shape[-1]), dtype=jnp.float32)
    angles = positions.astype(jnp.float32)[..., None] * inverse
    cosine = jnp.cos(angles)
    sine_part = jnp.sin(angles)
    front_half = vectors[..., :half_width]
    back_half = vectors[..., half_width:]
    return jnp.concatenate(
        [front_half * cosine - back_half * sine_part, back_half * cosine + front_half * sine_part],
        axis=-1,
    )


def arrange(columns, tp_count):
    lead = columns.shape[:-1]
    per_rank = HQ // tp_count
    query_part = columns[..., : HQ * HD].reshape(lead + (tp_count, per_rank * HD))
    key_part = jnp.repeat(
        columns[..., HQ * HD : (HQ + KVH) * HD].reshape(lead + (KVH, HD)), tp_count // KVH, axis=-2
    )
    value_part = jnp.repeat(
        columns[..., (HQ + KVH) * HD :].reshape(lead + (KVH, HD)), tp_count // KVH, axis=-2
    )
    return jnp.concatenate([query_part, key_part, value_part], axis=-1)


def arrange_tiles(qkv_rows, out_rows):
    rows = qkv_rows.shape[0]
    tiles = jnp.concatenate([qkv_rows, out_rows], axis=1).reshape(rows, 40, HD)
    order = [[2 * t, 2 * t + 1, 16 + t // 2, 20 + t // 2, 24 + 2 * t, 25 + 2 * t] for t in range(8)]
    picked = jnp.stack([jnp.stack([tiles[:, k] for k in row]) for row in order])
    return picked.reshape(8, 6, GROUPS, 4, HD)


def normalize(row_block, norm_gain):
    wide_rows = row_block.astype(jnp.float32)
    scaled = wide_rows * lax.rsqrt(
        jnp.mean(wide_rows * wide_rows, axis=1, keepdims=True) + norm_eps
    )
    return (scaled * norm_gain.astype(jnp.float32)).astype(jnp.bfloat16)


def combine_partial(earlier, later):
    top_score = jnp.maximum(earlier[0], later[0])
    left_factor = jnp.exp(earlier[0] - top_score)
    right_factor = jnp.exp(later[0] - top_score)
    return (
        top_score,
        earlier[1] * left_factor + later[1] * right_factor,
        earlier[2] * left_factor[..., None] + later[2] * right_factor[..., None],
    )


def body(
    hidden,
    norm_gain,
    qkv_bias,
    qkv_weight,
    out_weight,
    key_cache,
    value_cache,
    cache_len,
    block_pos,
):
    tp_count = lax.axis_size(TP)
    tp_index = lax.axis_index(TP)
    head_cols = out_weight.shape[1]
    rollouts = hidden.shape[0]
    group_size = HQ // KVH
    score_scale = HD ** (-0.5)
    per_rank = HQ // tp_count
    served_width = (per_rank + 2) * HD
    head_width = head_cols // tp_count
    src = arrange_tiles(qkv_weight, out_weight)
    joint = relay(src).reshape(6, 3584, HD)
    served_qkv = jnp.moveaxis(joint[:4], 0, 1).reshape(3584, served_width)
    served_out = jnp.moveaxis(joint[4:], 0, 1).reshape(3584, head_width)
    bias_wide = qkv_bias.astype(jnp.float32)
    normed = normalize(hidden, norm_gain)
    bias_grouped = arrange(bias_wide, tp_count)
    own_bias = lax.dynamic_slice_in_dim(bias_grouped, tp_index, 1, 0).reshape(served_width)
    local_cols = jnp.dot(normed, served_qkv, preferred_element_type=jnp.float32) + own_bias
    gathered = gather_directly(local_cols.astype(jnp.bfloat16), TP, 1)
    grouped_cols = gathered.reshape(rollouts, tp_count, served_width)
    repeat_count = tp_count // KVH
    queries = grouped_cols[:, :, : per_rank * HD].reshape(rollouts, HQ, HD).astype(jnp.float32)
    new_keys = grouped_cols[:, ::repeat_count, per_rank * HD : (per_rank + 1) * HD].astype(
        jnp.float32
    )
    fresh_value = grouped_cols[:, ::repeat_count, (per_rank + 1) * HD :]
    intra_pos = cache_len % STRETCH
    fresh_key = rotate(new_keys, jnp.broadcast_to(intra_pos[:, None], (rollouts, KVH))).astype(
        jnp.bfloat16
    )
    self_query = rotate(queries, jnp.broadcast_to(intra_pos[:, None], (rollouts, HQ))).astype(
        jnp.bfloat16
    )
    self_score = score_scale * jnp.einsum(
        "rkgd,rkd->rkg",
        self_query.reshape(rollouts, KVH, group_size, HD),
        fresh_key,
        preferred_element_type=jnp.float32,
    )
    blocks = block_pos.shape[1]
    block_query = rotate(
        queries[:, None], jnp.broadcast_to(block_pos[:, :, None], (rollouts, blocks, HQ))
    ).astype(jnp.bfloat16)
    cached_keys = key_cache.reshape(rollouts, blocks, BLOCK, KVH, HD)
    cached_values = value_cache.reshape(rollouts, blocks, BLOCK, KVH, HD)
    scores = score_scale * jnp.einsum(
        "rbkgd,rbpkd->rkgbp",
        block_query.reshape(rollouts, blocks, KVH, group_size, HD),
        cached_keys,
        preferred_element_type=jnp.float32,
    )
    shard_start = lax.axis_index(SEQ_TP) * key_cache.shape[1]
    positions = shard_start + jnp.arange(key_cache.shape[1], dtype=jnp.int32).reshape(blocks, BLOCK)
    valid_mask = (positions[None] < cache_len[:, None, None])[:, None, None]
    masked = jnp.where(valid_mask, scores, floor_score)
    local_max = jnp.max(masked, axis=(3, 4))
    weights = jnp.where(valid_mask, jnp.exp(masked - local_max[..., None, None]), 0.0)
    local_sum = jnp.sum(weights, axis=(3, 4))
    local_out = jnp.einsum(
        "rkgbp,rbpkd->rkgd",
        weights.astype(jnp.bfloat16),
        cached_values,
        preferred_element_type=jnp.float32,
    )
    total_max, total_sum, total_out = combined_by_axis(
        (local_max, local_sum, local_out), SEQ_TP, combine_partial
    )
    top_score = jnp.maximum(total_max, self_score)
    old_factor = jnp.exp(total_max - top_score)
    fresh_weight = jnp.exp(self_score - top_score)
    fresh_rounded = lax.optimization_barrier(fresh_weight.astype(jnp.bfloat16)).astype(jnp.float32)
    denominator = total_sum * old_factor + fresh_weight
    numerator = (
        total_out * old_factor[..., None]
        + fresh_rounded[..., None] * fresh_value.astype(jnp.float32)[:, :, None, :]
    )
    attention = (numerator / denominator[..., None]).reshape(rollouts, HQ * HD).astype(jnp.bfloat16)
    own_heads = lax.dynamic_slice_in_dim(attention, tp_index * head_width, head_width, 1)
    partial_out = lax.dot_general(
        own_heads, served_out, (((1,), (1,)), ((), ())), preferred_element_type=jnp.float32
    )
    attended = of_everyone(partial_out, TP).astype(jnp.bfloat16)
    fresh_kv = jnp.concatenate(
        [fresh_key.reshape(rollouts, KVH * HD), fresh_value.reshape(rollouts, KVH * HD)], axis=1
    )
    return (attended, fresh_kv, served_qkv, served_out)


def solution(mesh):
    finer = Mesh(
        mesh.devices.reshape(2, 4, 4, 2, mesh.shape["roll"]),
        ("seq_0", "seq_1", "tp_0", "tp_1", "roll"),
    )
    in_specs = (
        P("roll", None),
        P(),
        P(),
        P(SEQ_TP_ROLL, None),
        P(SEQ_TP_ROLL, None),
        P("roll", SEQ_TP, None),
        P("roll", SEQ_TP, None),
        P("roll"),
        P("roll", SEQ_TP),
    )
    out_specs = (P("roll", None), P("roll", None), P(None, TP), P(None, TP))
    return jax.shard_map(body, mesh=finer, in_specs=in_specs, out_specs=out_specs, check_vma=False)
```

```python
import jax
import jax.numpy as jnp
import numpy as np
from jax import lax
from jax.experimental import pallas as pl
from jax.experimental.pallas import tpu as pltpu
from jax.sharding import Mesh
from jax.sharding import PartitionSpec as P

HQ = 16
KVH = 4
HD = 128
BLOCK = 512
STRETCH = 8192
ROWS = 28
GROUPS = 7
HERE = 1024
TP = ("tp_0", "tp_1")
SEQ = ("seq_0", "seq_1")
SEQ_TP = ("seq_0", "seq_1", "tp_0", "tp_1")
SEQ_TP_ROLL = ("seq_0", "seq_1", "tp_0", "tp_1", "roll")
MESH = pl.DeviceIdType.MESH
F32 = jnp.float32
BF16 = jnp.bfloat16

rope_base = 10000000.0
norm_eps = 1e-06
lowest = -1e30
floor_top = -1e20


def frequencies(width):
    half_width = width // 2
    exact = rope_base ** (-2.0 * np.arange(half_width) / width)
    octave = np.floor(np.log2(exact))
    quantum = 2.0 ** (8.0 - octave)
    return np.floor(exact * quantum) / quantum


def normalize(row_block, norm_gain):
    wide_rows = row_block.astype(F32)
    scaled = wide_rows * lax.rsqrt(
        jnp.mean(wide_rows * wide_rows, axis=1, keepdims=True) + norm_eps
    )
    return (scaled * norm_gain.astype(F32)).astype(BF16)


def device(x, y, z, core):
    return (x % 2, z, y, core, x // 2)


ORDER = (0, -1, 1, 2)
TP_STEPS = tuple((dy, dc) for dy in (0, 3, 1, 2) for dc in (0, 1))
PLANE_STEPS = tuple((dx, dz) for dx in (2, 1, 3, 0) for dz in (2, 1, 3, 0))


def layer_kernel(
    tiles_ref, normed_ref, bias_ref, turn_ref, len_ref, key_ref, value_ref,
    w_ref, fresh_ref, final_ref,
    kbuf, vbuf, other, wq, part, r2, qb, rot, self_s, s_buf, p_buf, ob, r5, c6, r6, po, r7,
    cache_sem, own_sem, trade_send, trade_recv, ring_send, ring_recv, pair_sem, other_sem,
    stage_send, recv2, recv3, recv5, recv6, recv7, recv8,
):
    x = lax.axis_index("roll") * 2 + lax.axis_index("seq_0")
    y, z, core = lax.axis_index("tp_0"), lax.axis_index("seq_1"), lax.axis_index("tp_1")
    seq, roll, tp = (x % 2) * 4 + z, x // 2, y * 2 + core

    def remote(src, dst, send, recv, target):
        return pltpu.make_async_remote_copy(
            src_ref=src, dst_ref=dst, send_sem=send, recv_sem=recv,
            device_id=device(*target), device_id_type=MESH,
        )

    def tp_peer(dy, dc):
        return (x, (y + dy) % 4, z, (core + dc) % 2)

    def plane_peer(dx, dz):
        return ((x + dx) % 4, y, (z + dz) % 4, core)

    partners = [tp_peer(dy, dc) for dy, dc in TP_STEPS if (dy, dc) != (0, 0)]
    partners += [plane_peer(dx, dz) for dx, dz in PLANE_STEPS if (dx, dz) != (0, 0)]

    caches = []
    for r in range(4):
        caches.append(pltpu.make_async_copy(key_ref.at[r], kbuf.at[r], cache_sem.at[0, r]))
    for r in range(4):
        caches.append(pltpu.make_async_copy(value_ref.at[r], vbuf.at[r], cache_sem.at[1, r]))

    barrier = pltpu.get_barrier_semaphore()
    for partner in partners:
        pl.semaphore_signal(barrier, inc=1, device_id=device(*partner), device_id_type=MESH)

    def tiles_of(kind, ty, tcore):
        t = ty * 2 + tcore
        return (24 + 2 * t, 2) if kind == 0 else (2 * t, 2) if kind == 1 else (16 + 4 * tcore + ty, 1)

    def place_of(kind, tcore):
        return (0, 2) if kind == 0 else (2, 2) if kind == 1 else (4 + tcore, 1)

    def traded(kind, dy, dc):
        ty, tcore = (y + dy) % 4, (core + dc) % 2
        first, count = tiles_of(kind, ty, tcore)
        to, _ = place_of(kind, tcore)
        src = tiles_ref.at[pl.ds(first, count)]
        dst = w_ref.at[pl.ds(to, count), seq, tp, roll]
        if (dy, dc) == (0, 0):
            return pltpu.make_async_copy(src, dst, own_sem.at[kind])
        return remote(src, dst, trade_send.at[kind], trade_recv.at[kind, dy * 2 + dc], (x, ty, z, tcore))

    def got_trade(kind):
        to, count = place_of(kind, core)
        for dy, dc in TP_STEPS:
            if (dy, dc) == (0, 0):
                traded(kind, 0, 0).wait()
            else:
                source = ((y - dy) % 4) * 2 + (core + dc) % 2
                here = w_ref.at[pl.ds(to, count), seq, source, roll]
                remote(here, here, trade_send.at[kind], trade_recv.at[kind, dy * 2 + dc], tp_peer(dy, dc)).wait_recv()

    for kind in range(3):
        traded(kind, 0, 0).start()
    pl.semaphore_wait(barrier, len(partners))

    across = remote(normed_ref.at[1], other, other_sem.at[0], other_sem.at[1], plane_peer(2, 0))
    across.start()
    for kind in range(3):
        for dy, dc in TP_STEPS:
            if (dy, dc) != (0, 0):
                traded(kind, dy, dc).start()
    for copy in caches:
        copy.start()

    def region(kind, half):
        if kind < 2:
            return kind * 2 + half, 0, 8
        return 4 + core, half * 4, 4

    def block_at(kind, half, bx, bz, part_of):
        tile, first, count = region(kind, half)
        if part_of is not None:
            count = count // 2
            first = first + part_of * count
        return w_ref.at[pl.ds(tile, 1), (bx % 2) * 4 + bz, pl.ds(first, count), bx // 2]

    def coords(half, f, g):
        return ((x + g) % 4, (z + f) % 4) if half == 0 else ((x + f) % 4, (z + g) % 4)

    def ring(kind, half, message, f, g, part_of, step):
        bx, bz = coords(half, f, g)
        tx, tz = coords(half, *step)
        block = block_at(kind, half, bx, bz, part_of)
        return remote(block, block, ring_send.at[kind], ring_recv.at[kind, half * 20 + message], (tx, y, tz, core))

    def to_pair(kind, half, f, g, part_of=None):
        if kind == 2:
            bx, bz = coords(half, f, g)
            block = block_at(kind, half, bx, bz, part_of)
            remote(block, block, pair_sem.at[0], pair_sem.at[1], tp_peer(0, 1)).start()

    def sideways(kind, half, f):
        k = 4 + ORDER.index(f) * 4
        ring(kind, half, k, f, 0, None, (0, 1)).start()
        ring(kind, half, k + 1, f, 0, None, (0, -1)).start()

    def s1(kind):
        for half in (0, 1):
            ring(kind, half, 0, 0, 0, None, (1, 0)).start()
            ring(kind, half, 1, 0, 0, None, (-1, 0)).start()
        for half in (0, 1):
            sideways(kind, half, 0)
            to_pair(kind, half, 0, 0)

    def s2(kind):
        for half in (0, 1):
            ring(kind, half, 0, -1, 0, None, (1, 0)).wait_recv()
            ring(kind, half, 2, -1, 0, 0, (1, 0)).start()
            ring(kind, half, 1, 1, 0, None, (1, 0)).wait_recv()
            ring(kind, half, 3, 1, 0, 1, (-1, 0)).start()
        for half in (0, 1):
            for f in (-1, 1):
                sideways(kind, half, f)
                to_pair(kind, half, f, 0)

    def s3(kind):
        for half in (0, 1):
            ring(kind, half, 2, 2, 0, 0, (1, 0)).wait_recv()
            ring(kind, half, 3, 2, 0, 1, (1, 0)).wait_recv()
            sideways(kind, half, 2)
            to_pair(kind, half, 2, 0)

    def s4(kind, fs=ORDER):
        for f in fs:
            for half in (0, 1):
                k = 4 + ORDER.index(f) * 4
                ring(kind, half, k, f, -1, None, (0, 1)).wait_recv()
                ring(kind, half, k + 2, f, -1, 0, (0, 1)).start()
                to_pair(kind, half, f, -1)
                ring(kind, half, k + 1, f, 1, None, (0, 1)).wait_recv()
                ring(kind, half, k + 3, f, 1, 1, (0, -1)).start()
                to_pair(kind, half, f, 1)

    def s5(kind):
        for f in ORDER:
            for half in (0, 1):
                k = 4 + ORDER.index(f) * 4
                ring(kind, half, k + 2, f, 2, 0, (0, 1)).wait_recv()
                to_pair(kind, half, f, 2, 0)
                ring(kind, half, k + 3, f, 2, 1, (0, 1)).wait_recv()
                to_pair(kind, half, f, 2, 1)
        sent = w_ref.at[0:5, 0 : (6 if kind < 2 else 3), :, 0]
        remote(sent, sent, ring_send.at[kind], ring_recv.at[kind, 0], plane_peer(0, 1)).wait_send()

    def tp_send(stage, src_of, dst, sems):
        for dy, dc in TP_STEPS:
            if (dy, dc) != (0, 0):
                target = tp_peer(dy, dc)
                remote(src_of(target[1] * 2 + target[3]), dst, stage_send.at[stage], sems.at[dy * 2 + dc], target).start()

    def tp_wait(stage, buffer, sems):
        for dy, dc in TP_STEPS:
            if (dy, dc) != (0, 0):
                here = buffer.at[((y - dy) % 4) * 2 + (core + dc) % 2]
                remote(here, here, stage_send.at[stage], sems.at[dy * 2 + dc], tp_peer(dy, dc)).wait_recv()

    def sent_all(stage, buffer, count):
        sent = buffer.at[0:count]
        remote(sent, sent, stage_send.at[stage], recv3.at[0], tp_peer(0, 1)).wait_send()

    def project():
        got_trade(1)
        got_trade(2)
        across.wait_recv()
        for k in range(3):
            tile = (2 + k) if k < 2 else 4 + core
            rows = w_ref[tile, seq, :, roll]
            wq[:, k * HD : (k + 1) * HD] = rows.reshape(8 * ROWS, HD)
        for k, lhs in ((0, normed_ref[0]), (1, other[...])):
            made = jnp.dot(lhs, wq[...], preferred_element_type=F32)
            part[k] = made[0:4]
        r2[x * 4 + z] = part[0]
        for dx, dz in PLANE_STEPS:
            if (dx, dz) != (0, 0):
                tx, _, tz, _ = plane_peer(dx, dz)
                remote(
                    part.at[(tx // 2 + roll) % 2], r2.at[x * 4 + z], stage_send.at[0],
                    recv2.at[dx * 4 + dz], (tx, y, tz, core),
                ).start()

    def share():
        for dx, dz in PLANE_STEPS:
            if (dx, dz) != (0, 0):
                here = r2.at[((x - dx) % 4) * 4 + (z - dz) % 4]
                remote(here, here, stage_send.at[0], recv2.at[dx * 4 + dz], plane_peer(dx, dz)).wait_recv()
        total = r2[0]
        for k in range(1, 16):
            total = total + r2[k]
        for k in range(3):
            row = (2 * tp + k) if k < 2 else 16 + 4 * core + y
            qb[tp, k] = (total[:, k * HD : (k + 1) * HD] + bias_ref[row]).astype(BF16)
        tp_send(1, lambda t: qb.at[tp], qb.at[tp], recv3)

    def turn(v, position):
        return v * turn_ref[position, 0] + pltpu.roll(v, 64, v.ndim - 1) * turn_ref[position, 1]

    def queries():
        tp_wait(1, qb, recv3)
        for g in range(KVH):
            fresh_key = turn(qb[2 * g, 2].astype(F32), 0).astype(BF16)
            fresh_ref[:, g * HD : (g + 1) * HD] = fresh_key
            fresh_ref[:, (KVH + g) * HD : (KVH + g + 1) * HD] = qb[2 * g + 1, 2]
            for h in range(4 * g, 4 * g + 4):
                q = qb[h // 2, h % 2].astype(F32)
                own = turn(q, 0).astype(BF16).astype(F32)
                score = jnp.sum(own * fresh_key.astype(F32), axis=1, keepdims=True) * HD ** (-0.5)
                self_s[4 * h : 4 * h + 4] = jnp.broadcast_to(score, (4, HD))
                for b in range(2):
                    rot[b, 4 * h : 4 * h + 4] = turn(q, 1 + b)

    def scores():
        start = (seq * 8 + tp) * HERE
        owner = lax.broadcasted_iota(jnp.int32, (16, BLOCK), 0) % 4
        column = lax.broadcasted_iota(jnp.int32, (16, BLOCK), 1)
        for r in range(4):
            caches[r].wait()
            for b in range(2):
                valid = (owner == r) & (column + (start + b * BLOCK) < len_ref[r])
                for g in range(KVH):
                    rows, cols = slice(16 * g, 16 * g + 16), slice(b * BLOCK, (b + 1) * BLOCK)
                    made = lax.dot_general(
                        rot[b, rows].astype(BF16), kbuf[r, cols, g * HD : (g + 1) * HD],
                        (((1,), (1,)), ((), ())), preferred_element_type=F32,
                    )
                    before = s_buf[rows, cols] if r > 0 else jnp.full((16, BLOCK), lowest, F32)
                    s_buf[rows, cols] = jnp.where(valid, made * HD ** (-0.5), before)

    def values():
        for g in range(KVH):
            s = s_buf[16 * g : 16 * g + 16]
            top = jnp.maximum(jnp.max(s, axis=1, keepdims=True), floor_top)
            w = jnp.exp(s - top)
            p_buf[16 * g : 16 * g + 16] = w.astype(BF16)
            low = jnp.sum(w, axis=1, keepdims=True)
            for k in range(2):
                rows = slice(8 * k, 8 * k + 8)
                ob[2 * g + k, 0] = jnp.broadcast_to(top[rows], (8, HD))
                ob[2 * g + k, 1] = jnp.broadcast_to(low[rows], (8, HD))
        owner = lax.broadcasted_iota(jnp.int32, (16, HERE), 0) % 4
        for r in range(4):
            caches[4 + r].wait()
        for g in range(KVH):
            total = jnp.zeros((16, HD), F32)
            w = p_buf[16 * g : 16 * g + 16].astype(F32)
            for r in range(4):
                mine = jnp.where(owner == r, w, 0.0).astype(BF16)
                total += jnp.dot(mine, vbuf[r, :, g * HD : (g + 1) * HD], preferred_element_type=F32)
            ob[2 * g, 2] = total[0:8]
            ob[2 * g + 1, 2] = total[8:16]
        r5[tp] = ob[tp]
        tp_send(2, lambda t: ob.at[t], r5.at[tp], recv5)

    def combined(buffer):
        top = buffer[0, 0]
        for k in range(1, 8):
            top = jnp.maximum(top, buffer[k, 0])
        low, out = jnp.zeros_like(top), jnp.zeros_like(top)
        for k in range(8):
            factor = jnp.exp(buffer[k, 0] - top)
            low += buffer[k, 1] * factor
            out += buffer[k, 2] * factor
        return top, low, out

    def over_tp():
        tp_wait(2, r5, recv5)
        for k, value in enumerate(combined(r5)):
            c6[k] = value
            r6[seq, k] = value
        for dl in range(2):
            for dz in (2, 1, 3, 0):
                if dl + dz > 0:
                    tx, tz = roll * 2 + (x + dl) % 2, (z + dz) % 4
                    remote(c6, r6.at[seq], stage_send.at[3], recv6.at[dl * 4 + dz], (tx, y, tz, core)).start()

    def finish():
        for dl in range(2):
            for dz in (2, 1, 3, 0):
                if dl + dz > 0:
                    here = r6.at[((x + dl) % 2) * 4 + (z - dz) % 4]
                    remote(here, here, stage_send.at[3], recv6.at[dl * 4 + dz], plane_peer(0, 1)).wait_recv()
        old_top, old_low, old_out = combined(r6)
        mine = self_s[pl.ds(pl.multiple_of(tp * 8, 8), 8)]
        top = jnp.maximum(old_top, mine)
        factor, fresh = jnp.exp(old_top - top), jnp.exp(mine - top)
        own_value = qb[(tp // 2) * 2 + 1, 2].astype(F32)
        both = jnp.concatenate([own_value, own_value], axis=0)
        numerator = old_out * factor + fresh.astype(BF16).astype(F32) * both
        attention = (numerator / (old_low * factor + fresh)).astype(BF16)
        return attention

    def out_project(attention):
        for o in range(8):
            sums = []
            for k in range(2):
                rows = w_ref[k, o].reshape(16 * ROWS, HD)
                sums.append(lax.dot_general(attention, rows, (((1,), (1,)), ((), ())), preferred_element_type=F32))
            po[o, :, 0:448] = sums[0][0:4] + sums[1][4:8]
            po[o, :, 448:512] = jnp.zeros((4, 64), F32)
        r7[tp] = po[tp]
        tp_send(4, lambda t: po.at[t], r7.at[tp], recv7)

    def reduce_out():
        tp_wait(4, r7, recv7)
        total = r7[0]
        for k in range(1, 8):
            total = total + r7[k]
        final_ref[tp] = total.astype(BF16)
        tp_send(5, lambda t: final_ref.at[tp], final_ref.at[tp], recv8)

    got_trade(0)
    s1(0)
    project()
    s1(1)
    s2(0)
    share()
    s3(0)
    s1(2)
    queries()
    s2(1)
    scores()
    s4(0)
    values()
    s3(1)
    s2(2)
    over_tp()
    s5(0)
    s4(1)
    out_project(finish())
    s3(2)
    s4(2)
    reduce_out()
    s5(1)
    s5(2)
    tile = w_ref.at[5 - core]
    whole = remote(tile, tile, pair_sem.at[0], pair_sem.at[1], tp_peer(0, 1))
    whole.wait_send()
    whole.wait_recv()
    tp_wait(5, final_ref, recv8)
    for kind in range(3):
        sent = tiles_ref.at[0 : (14 if kind < 2 else 7)]
        remote(sent, sent, trade_send.at[kind], trade_recv.at[kind, 1], tp_peer(0, 1)).wait_send()
    across.wait_send()
    sent_all(0, r2, 15)
    sent_all(1, qb, 7)
    sent_all(2, ob, 7)
    sent_all(3, r6, 7)
    sent_all(4, po, 7)
    sent_all(5, final_ref, 7)


def layer(tiles, normed, bias, turns, lengths, keys, values):
    hbm, vmem = pl.BlockSpec(memory_space=pltpu.HBM), pl.BlockSpec(memory_space=pltpu.VMEM)
    smem, dma = pl.BlockSpec(memory_space=pltpu.SMEM), pltpu.SemaphoreType.DMA
    return pl.pallas_call(
        layer_kernel,
        name="layer",
        out_shape=(
            jax.ShapeDtypeStruct((6, 8, 8, 2, GROUPS, 4, HD), BF16),
            jax.ShapeDtypeStruct((4, 2 * KVH * HD), BF16),
            jax.ShapeDtypeStruct((8, 4, 512), BF16),
        ),
        in_specs=[hbm, vmem, vmem, vmem, smem, hbm, hbm],
        out_specs=(vmem, vmem, vmem),
        scratch_shapes=[
            pltpu.VMEM((4, HERE, KVH * HD), BF16),
            pltpu.VMEM((4, HERE, KVH * HD), BF16),
            pltpu.VMEM((8, 8 * ROWS), BF16),
            pltpu.VMEM((8 * ROWS, 3 * HD), BF16),
            pltpu.VMEM((2, 4, 3 * HD), F32),
            pltpu.VMEM((16, 4, 3 * HD), F32),
            pltpu.VMEM((8, 3, 4, HD), BF16),
            pltpu.VMEM((2, 64, HD), F32),
            pltpu.VMEM((64, HD), F32),
            pltpu.VMEM((64, HERE), F32),
            pltpu.VMEM((64, HERE), BF16),
            pltpu.VMEM((8, 3, 8, HD), F32),
            pltpu.VMEM((8, 3, 8, HD), F32),
            pltpu.VMEM((3, 8, HD), F32),
            pltpu.VMEM((8, 3, 8, HD), F32),
            pltpu.VMEM((8, 4, 512), F32),
            pltpu.VMEM((8, 4, 512), F32),
            dma((2, 4)), dma((3,)), dma((3,)), dma((3, 8)), dma((3,)), dma((3, 40)), dma((2,)), dma((2,)),
            dma((6,)), dma((16,)), dma((8,)), dma((8,)), dma((8,)), dma((8,)), dma((8,)),
        ],
        compiler_params=pltpu.CompilerParams(collective_id=0, has_side_effects=True, vmem_limit_bytes=36 * 2**20),
    )(tiles, normed, bias, turns, lengths, keys, values)


def body(
    hidden,
    norm_gain,
    qkv_bias,
    qkv_weight,
    out_weight,
    key_cache,
    value_cache,
    cache_len,
    block_pos,
):
    rollouts = hidden.shape[0]
    rows = jnp.concatenate([qkv_weight, out_weight], axis=1).reshape(ROWS, 40, HD)
    tiles = jnp.transpose(rows, (1, 0, 2)).reshape(40, GROUPS, 4, HD)
    normed = normalize(hidden, norm_gain)
    near = lax.dynamic_slice_in_dim(normed, lax.axis_index(SEQ) * 448, 448, 1)
    near = near.reshape(rollouts, 8, 2, ROWS)
    odd = lax.axis_index("roll") == 1
    even_rows, odd_rows = (near[:, :, k].reshape(rollouts, 8 * ROWS) for k in (0, 1))
    chosen = jnp.stack([jnp.where(odd, odd_rows, even_rows), jnp.where(odd, even_rows, odd_rows)])
    chosen = jnp.pad(chosen, ((0, 0), (0, 4), (0, 0)))
    bias = qkv_bias.astype(F32).reshape(24, 1, HD)
    inverse = jnp.asarray(frequencies(HD), dtype=F32)
    positions = jnp.concatenate([(cache_len % STRETCH)[:, None], block_pos], axis=1)
    angles = positions.T.astype(F32)[..., None] * inverse
    cosine, sine = jnp.cos(angles), jnp.sin(angles)
    turns = jnp.stack(
        [jnp.concatenate([cosine, cosine], axis=-1), jnp.concatenate([-sine, sine], axis=-1)], axis=1
    )
    w, fresh_kv, final = layer(tiles, chosen, bias, turns, cache_len, key_cache, value_cache)
    joint = w.reshape(6, 3584, HD)
    served_out = jnp.moveaxis(joint[:2], 0, 1).reshape(3584, 2 * HD)
    served_qkv = jnp.moveaxis(joint[2:], 0, 1).reshape(3584, 4 * HD)
    attended = jnp.moveaxis(final[:, :, :448], 0, 1).reshape(rollouts, 3584)
    return (attended, fresh_kv, served_qkv, served_out)


def solution(mesh):
    finer = Mesh(
        mesh.devices.reshape(2, 4, 4, 2, mesh.shape["roll"]),
        ("seq_0", "seq_1", "tp_0", "tp_1", "roll"),
    )
    in_specs = (
        P("roll", None),
        P(),
        P(),
        P(SEQ_TP_ROLL, None),
        P(SEQ_TP_ROLL, None),
        P("roll", SEQ_TP, None),
        P("roll", SEQ_TP, None),
        P("roll"),
        P("roll", SEQ_TP),
    )
    out_specs = (P("roll", None), P("roll", None), P(None, TP), P(None, TP))
    return jax.shard_map(body, mesh=finer, in_specs=in_specs, out_specs=out_specs, check_vma=False)
```

```python
import jax
import jax.numpy as jnp
import numpy as np
from jax import lax
from jax.experimental import pallas as pl
from jax.experimental.pallas import tpu as pltpu
from jax.sharding import Mesh
from jax.sharding import PartitionSpec as P

HQ = 16
KVH = 4
HD = 128
BLOCK = 512
STRETCH = 8192
ROWS = 28
GROUPS = 7
HERE = 1024
TP = ("tp_0", "tp_1")
SEQ = ("seq_0", "seq_1")
SEQ_TP = ("seq_0", "seq_1", "tp_0", "tp_1")
SEQ_TP_ROLL = ("seq_0", "seq_1", "tp_0", "tp_1", "roll")
MESH = pl.DeviceIdType.MESH
F32 = jnp.float32
BF16 = jnp.bfloat16

rope_base = 10000000.0
norm_eps = 1e-06
lowest = -1e30
floor_top = -1e20


def frequencies(width):
    half_width = width // 2
    exact = rope_base ** (-2.0 * np.arange(half_width) / width)
    octave = np.floor(np.log2(exact))
    quantum = 2.0 ** (8.0 - octave)
    return np.floor(exact * quantum) / quantum


def device(x, y, z, core):
    return (x % 2, z, y, core, x // 2)


ORDER = (0, -1, 1, 2)
TP_STEPS = tuple((dy, dc) for dy in (0, 3, 1, 2) for dc in (0, 1))
PLANE_STEPS = tuple((dx, dz) for dx in (2, 1, 3, 0) for dz in (2, 1, 3, 0))


def layer_kernel(
    hidden_ref, gain_ref, bias_hbm, qkv_ref, out_ref, len_ref, pos_ref, key_ref, value_ref,
    w_ref, fresh_ref, final_ref,
    hidden_in, gain_in, bias_in, qkv_in, out_in, tiles_ref, near, bias_ref, turn_ref,
    kbuf, vbuf, normed_ref, other, wq, part, r2, qb, rot, self_s, s_buf, p_buf, ob, r5, c6, r6, po, r7,
    load_sem, cache_sem, trade_send, trade_recv, ring_send, ring_recv, pair_sem, other_sem,
    stage_send, recv2, recv3, recv5, recv6, recv7, recv8,
):
    x = lax.axis_index("roll") * 2 + lax.axis_index("seq_0")
    y, z, core = lax.axis_index("tp_0"), lax.axis_index("seq_1"), lax.axis_index("tp_1")
    seq, roll, tp = (x % 2) * 4 + z, x // 2, y * 2 + core

    def remote(src, dst, send, recv, target):
        return pltpu.make_async_remote_copy(
            src_ref=src, dst_ref=dst, send_sem=send, recv_sem=recv,
            device_id=device(*target), device_id_type=MESH,
        )

    def tp_peer(dy, dc):
        return (x, (y + dy) % 4, z, (core + dc) % 2)

    def plane_peer(dx, dz):
        return ((x + dx) % 4, y, (z + dz) % 4, core)

    partners = [tp_peer(dy, dc) for dy, dc in TP_STEPS if (dy, dc) != (0, 0)]
    partners += [plane_peer(dx, dz) for dx, dz in PLANE_STEPS if (dx, dz) != (0, 0)]

    caches = []
    for r in range(4):
        caches.append(pltpu.make_async_copy(key_ref.at[r], kbuf.at[r], cache_sem.at[0, r]))
    for r in range(4):
        caches.append(pltpu.make_async_copy(value_ref.at[r], vbuf.at[r], cache_sem.at[1, r]))

    barrier = pltpu.get_barrier_semaphore()
    for partner in partners:
        pl.semaphore_signal(barrier, inc=1, device_id=device(*partner), device_id_type=MESH)
    loads = [
        pltpu.make_async_copy(src, dst, load_sem.at[k])
        for k, (src, dst) in enumerate((
            (out_ref, out_in), (qkv_ref, qkv_in), (hidden_ref, hidden_in), (gain_ref, gain_in), (bias_hbm, bias_in),
        ))
    ]
    for copy in loads:
        copy.start()

    def stage(source, first, count):
        for k in range(count):
            tiles_ref[first + k] = source[:, k * HD : (k + 1) * HD].reshape(GROUPS, 4, HD)

    def select_rows():
        wide = hidden_in[...].astype(F32)
        scale = lax.rsqrt(jnp.sum(wide * wide, axis=1, keepdims=True) * (1.0 / 3584) + norm_eps)
        base = pl.multiple_of(((7 * seq) // 2) * HD, HD)
        wide = hidden_in[:, pl.ds(base, 512)].astype(F32) * scale * gain_in[:, pl.ds(base, 512)].astype(F32)
        near[0:4] = wide
        near[4:8] = jnp.zeros((4, 512), F32)
        lhs = near[...].astype(BF16)
        feature = lax.broadcasted_iota(jnp.int32, (512, 8 * ROWS), 0) + (base - seq * 448)
        column = lax.broadcasted_iota(jnp.int32, (512, 8 * ROWS), 1)
        wanted = column + (column // ROWS) * ROWS
        for k, r in ((0, roll), (1, 1 - roll)):
            picked = jnp.where(feature == wanted + r * ROWS, 1.0, 0.0).astype(BF16)
            normed_ref[k] = jnp.dot(lhs, picked, preferred_element_type=F32).astype(BF16)

    def tables():
        lane = lax.broadcasted_iota(jnp.int32, (4, HD), 1)
        row = lax.broadcasted_iota(jnp.int32, (4, HD), 0)
        freq = jnp.zeros((4, HD), F32)
        for k, value in enumerate(frequencies(HD)):
            freq = jnp.where(lane % 64 == k, jnp.float32(value), freq)
        for k in range(3):
            position = jnp.zeros((4, HD), jnp.int32)
            for r in range(4):
                here = len_ref[r] % STRETCH if k == 0 else pos_ref[r, k - 1]
                position = jnp.where(row == r, here, position)
            angle = position.astype(F32) * freq
            turn_ref[k, 0] = jnp.cos(angle)
            sine = jnp.sin(angle)
            turn_ref[k, 1] = jnp.where(lane < 64, -sine, sine)

    def tiles_of(kind, ty, tcore):
        t = ty * 2 + tcore
        return (24 + 2 * t, 2) if kind == 0 else (2 * t, 2) if kind == 1 else (16 + 4 * tcore + ty, 1)

    def place_of(kind, tcore):
        return (0, 2) if kind == 0 else (2, 2) if kind == 1 else (4 + tcore, 1)

    def traded(kind, dy, dc):
        ty, tcore = (y + dy) % 4, (core + dc) % 2
        first, count = tiles_of(kind, ty, tcore)
        to, _ = place_of(kind, tcore)
        src = tiles_ref.at[pl.ds(first, count)]
        dst = w_ref.at[pl.ds(to, count), seq, tp, roll]
        return remote(src, dst, trade_send.at[kind], trade_recv.at[kind, dy * 2 + dc], (x, ty, z, tcore))

    def got_trade(kind):
        to, count = place_of(kind, core)
        for dy, dc in TP_STEPS:
            if (dy, dc) != (0, 0):
                source = ((y - dy) % 4) * 2 + (core + dc) % 2
                here = w_ref.at[pl.ds(to, count), seq, source, roll]
                remote(here, here, trade_send.at[kind], trade_recv.at[kind, dy * 2 + dc], tp_peer(dy, dc)).wait_recv()

    def keep_own(kind):
        first, count = tiles_of(kind, y, core)
        to, _ = place_of(kind, core)
        for k in range(count):
            w_ref[to + k, seq, tp, roll] = tiles_ref[first + k]

    loads[0].wait()
    stage(out_in, 24, 16)
    keep_own(0)
    loads[1].wait()
    stage(qkv_in, 0, 24)
    keep_own(1)
    keep_own(2)
    for k in (2, 3, 4):
        loads[k].wait()
    select_rows()
    pl.semaphore_wait(barrier, len(partners))

    for dy, dc in TP_STEPS:
        if (dy, dc) != (0, 0):
            traded(0, dy, dc).start()
    across = remote(normed_ref.at[1], other, other_sem.at[0], other_sem.at[1], plane_peer(2, 0))
    across.start()
    for kind in (1, 2):
        for dy, dc in TP_STEPS:
            if (dy, dc) != (0, 0):
                traded(kind, dy, dc).start()
    for copy in caches:
        copy.start()
    tables()
    bias_ref[...] = bias_in[...].astype(F32)

    def region(kind, half):
        if kind < 2:
            return kind * 2 + half, 0, 8
        return 4 + core, half * 4, 4

    def block_at(kind, half, bx, bz, part_of):
        tile, first, count = region(kind, half)
        if part_of is not None:
            count = count // 2
            first = first + part_of * count
        return w_ref.at[pl.ds(tile, 1), (bx % 2) * 4 + bz, pl.ds(first, count), bx // 2]

    def coords(half, f, g):
        return ((x + g) % 4, (z + f) % 4) if half == 0 else ((x + f) % 4, (z + g) % 4)

    def ring(kind, half, message, f, g, part_of, step):
        bx, bz = coords(half, f, g)
        tx, tz = coords(half, *step)
        block = block_at(kind, half, bx, bz, part_of)
        return remote(block, block, ring_send.at[kind], ring_recv.at[kind, half * 20 + message], (tx, y, tz, core))

    def to_pair(kind, half, f, g, part_of=None):
        if kind == 2:
            bx, bz = coords(half, f, g)
            block = block_at(kind, half, bx, bz, part_of)
            remote(block, block, pair_sem.at[0], pair_sem.at[1], tp_peer(0, 1)).start()

    def sideways(kind, half, f):
        k = 4 + ORDER.index(f) * 4
        ring(kind, half, k, f, 0, None, (0, 1)).start()
        ring(kind, half, k + 1, f, 0, None, (0, -1)).start()

    def s1(kind):
        for half in (0, 1):
            ring(kind, half, 0, 0, 0, None, (1, 0)).start()
            ring(kind, half, 1, 0, 0, None, (-1, 0)).start()
        for half in (0, 1):
            sideways(kind, half, 0)
            to_pair(kind, half, 0, 0)

    def s2(kind):
        for half in (0, 1):
            ring(kind, half, 0, -1, 0, None, (1, 0)).wait_recv()
            ring(kind, half, 2, -1, 0, 0, (1, 0)).start()
            ring(kind, half, 1, 1, 0, None, (1, 0)).wait_recv()
            ring(kind, half, 3, 1, 0, 1, (-1, 0)).start()
        for half in (0, 1):
            for f in (-1, 1):
                sideways(kind, half, f)
                to_pair(kind, half, f, 0)

    def s3(kind):
        for half in (0, 1):
            ring(kind, half, 2, 2, 0, 0, (1, 0)).wait_recv()
            ring(kind, half, 3, 2, 0, 1, (1, 0)).wait_recv()
            sideways(kind, half, 2)
            to_pair(kind, half, 2, 0)

    def s4(kind, fs=ORDER):
        for f in fs:
            for half in (0, 1):
                k = 4 + ORDER.index(f) * 4
                ring(kind, half, k, f, -1, None, (0, 1)).wait_recv()
                ring(kind, half, k + 2, f, -1, 0, (0, 1)).start()
                to_pair(kind, half, f, -1)
                ring(kind, half, k + 1, f, 1, None, (0, 1)).wait_recv()
                ring(kind, half, k + 3, f, 1, 1, (0, -1)).start()
                to_pair(kind, half, f, 1)

    def s5(kind):
        for f in ORDER:
            for half in (0, 1):
                k = 4 + ORDER.index(f) * 4
                ring(kind, half, k + 2, f, 2, 0, (0, 1)).wait_recv()
                to_pair(kind, half, f, 2, 0)
                ring(kind, half, k + 3, f, 2, 1, (0, 1)).wait_recv()
                to_pair(kind, half, f, 2, 1)
        sent = w_ref.at[0:5, 0 : (6 if kind < 2 else 3), :, 0]
        remote(sent, sent, ring_send.at[kind], ring_recv.at[kind, 0], plane_peer(0, 1)).wait_send()

    def tp_send(stage, src_of, dst, sems):
        for dy, dc in TP_STEPS:
            if (dy, dc) != (0, 0):
                target = tp_peer(dy, dc)
                remote(src_of(target[1] * 2 + target[3]), dst, stage_send.at[stage], sems.at[dy * 2 + dc], target).start()

    def tp_wait(stage, buffer, sems):
        for dy, dc in TP_STEPS:
            if (dy, dc) != (0, 0):
                here = buffer.at[((y - dy) % 4) * 2 + (core + dc) % 2]
                remote(here, here, stage_send.at[stage], sems.at[dy * 2 + dc], tp_peer(dy, dc)).wait_recv()

    def sent_all(stage, buffer, count):
        sent = buffer.at[0:count]
        remote(sent, sent, stage_send.at[stage], recv3.at[0], tp_peer(0, 1)).wait_send()

    def project():
        got_trade(1)
        got_trade(2)
        across.wait_recv()
        for k in range(3):
            tile = (2 + k) if k < 2 else 4 + core
            rows = w_ref[tile, seq, :, roll]
            wq[:, k * HD : (k + 1) * HD] = rows.reshape(8 * ROWS, HD)
        for k, lhs in ((0, normed_ref[0]), (1, other[...])):
            made = jnp.dot(lhs, wq[...], preferred_element_type=F32)
            part[k] = made[0:4]
        r2[x * 4 + z] = part[0]
        for dx, dz in PLANE_STEPS:
            if (dx, dz) != (0, 0):
                tx, _, tz, _ = plane_peer(dx, dz)
                remote(
                    part.at[(tx // 2 + roll) % 2], r2.at[x * 4 + z], stage_send.at[0],
                    recv2.at[dx * 4 + dz], (tx, y, tz, core),
                ).start()

    def share():
        for dx, dz in PLANE_STEPS:
            if (dx, dz) != (0, 0):
                here = r2.at[((x - dx) % 4) * 4 + (z - dz) % 4]
                remote(here, here, stage_send.at[0], recv2.at[dx * 4 + dz], plane_peer(dx, dz)).wait_recv()
        total = r2[0]
        for k in range(1, 16):
            total = total + r2[k]
        for k in range(3):
            row = (2 * tp + k) if k < 2 else 16 + 4 * core + y
            qb[tp, k] = (total[:, k * HD : (k + 1) * HD] + bias_ref[pl.ds(row, 1)]).astype(BF16)
        tp_send(1, lambda t: qb.at[tp], qb.at[tp], recv3)

    def turn(v, position):
        return v * turn_ref[position, 0] + pltpu.roll(v, 64, v.ndim - 1) * turn_ref[position, 1]

    def queries():
        tp_wait(1, qb, recv3)
        for g in range(KVH):
            fresh_key = turn(qb[2 * g, 2].astype(F32), 0).astype(BF16)
            fresh_ref[:, g * HD : (g + 1) * HD] = fresh_key
            fresh_ref[:, (KVH + g) * HD : (KVH + g + 1) * HD] = qb[2 * g + 1, 2]
            for h in range(4 * g, 4 * g + 4):
                q = qb[h // 2, h % 2].astype(F32)
                own = turn(q, 0).astype(BF16).astype(F32)
                score = jnp.sum(own * fresh_key.astype(F32), axis=1, keepdims=True) * HD ** (-0.5)
                self_s[4 * h : 4 * h + 4] = jnp.broadcast_to(score, (4, HD))
                for b in range(2):
                    rot[b, 4 * h : 4 * h + 4] = turn(q, 1 + b)

    def scores():
        start = (seq * 8 + tp) * HERE
        owner = lax.broadcasted_iota(jnp.int32, (16, BLOCK), 0) % 4
        column = lax.broadcasted_iota(jnp.int32, (16, BLOCK), 1)
        for r in range(4):
            caches[r].wait()
            for b in range(2):
                valid = (owner == r) & (column + (start + b * BLOCK) < len_ref[r])
                for g in range(KVH):
                    rows, cols = slice(16 * g, 16 * g + 16), slice(b * BLOCK, (b + 1) * BLOCK)
                    made = lax.dot_general(
                        rot[b, rows].astype(BF16), kbuf[r, cols, g * HD : (g + 1) * HD],
                        (((1,), (1,)), ((), ())), preferred_element_type=F32,
                    )
                    before = s_buf[rows, cols] if r > 0 else jnp.full((16, BLOCK), lowest, F32)
                    s_buf[rows, cols] = jnp.where(valid, made * HD ** (-0.5), before)

    def values():
        for g in range(KVH):
            s = s_buf[16 * g : 16 * g + 16]
            top = jnp.maximum(jnp.max(s, axis=1, keepdims=True), floor_top)
            w = jnp.exp(s - top)
            p_buf[16 * g : 16 * g + 16] = w.astype(BF16)
            low = jnp.sum(w, axis=1, keepdims=True)
            for k in range(2):
                rows = slice(8 * k, 8 * k + 8)
                ob[2 * g + k, 0] = jnp.broadcast_to(top[rows], (8, HD))
                ob[2 * g + k, 1] = jnp.broadcast_to(low[rows], (8, HD))
        owner = lax.broadcasted_iota(jnp.int32, (16, HERE), 0) % 4
        for r in range(4):
            caches[4 + r].wait()
        for g in range(KVH):
            total = jnp.zeros((16, HD), F32)
            w = p_buf[16 * g : 16 * g + 16].astype(F32)
            for r in range(4):
                mine = jnp.where(owner == r, w, 0.0).astype(BF16)
                total += jnp.dot(mine, vbuf[r, :, g * HD : (g + 1) * HD], preferred_element_type=F32)
            ob[2 * g, 2] = total[0:8]
            ob[2 * g + 1, 2] = total[8:16]
        r5[tp] = ob[tp]
        tp_send(2, lambda t: ob.at[t], r5.at[tp], recv5)

    def combined(buffer):
        top = buffer[0, 0]
        for k in range(1, 8):
            top = jnp.maximum(top, buffer[k, 0])
        low, out = jnp.zeros_like(top), jnp.zeros_like(top)
        for k in range(8):
            factor = jnp.exp(buffer[k, 0] - top)
            low += buffer[k, 1] * factor
            out += buffer[k, 2] * factor
        return top, low, out

    def over_tp():
        tp_wait(2, r5, recv5)
        for k, value in enumerate(combined(r5)):
            c6[k] = value
            r6[seq, k] = value
        for dl in range(2):
            for dz in (2, 1, 3, 0):
                if dl + dz > 0:
                    tx, tz = roll * 2 + (x + dl) % 2, (z + dz) % 4
                    remote(c6, r6.at[seq], stage_send.at[3], recv6.at[dl * 4 + dz], (tx, y, tz, core)).start()

    def finish():
        for dl in range(2):
            for dz in (2, 1, 3, 0):
                if dl + dz > 0:
                    here = r6.at[((x + dl) % 2) * 4 + (z - dz) % 4]
                    remote(here, here, stage_send.at[3], recv6.at[dl * 4 + dz], plane_peer(0, 1)).wait_recv()
        old_top, old_low, old_out = combined(r6)
        mine = self_s[pl.ds(pl.multiple_of(tp * 8, 8), 8)]
        top = jnp.maximum(old_top, mine)
        factor, fresh = jnp.exp(old_top - top), jnp.exp(mine - top)
        own_value = qb[(tp // 2) * 2 + 1, 2].astype(F32)
        both = jnp.concatenate([own_value, own_value], axis=0)
        numerator = old_out * factor + fresh.astype(BF16).astype(F32) * both
        attention = (numerator / (old_low * factor + fresh)).astype(BF16)
        return attention

    def out_project(attention):
        for o in range(8):
            sums = []
            for k in range(2):
                rows = w_ref[k, o].reshape(16 * ROWS, HD)
                sums.append(lax.dot_general(attention, rows, (((1,), (1,)), ((), ())), preferred_element_type=F32))
            po[o, :, 0:448] = sums[0][0:4] + sums[1][4:8]
            po[o, :, 448:512] = jnp.zeros((4, 64), F32)
        r7[tp] = po[tp]
        tp_send(4, lambda t: po.at[t], r7.at[tp], recv7)

    def reduce_out():
        tp_wait(4, r7, recv7)
        total = r7[0]
        for k in range(1, 8):
            total = total + r7[k]
        final_ref[tp] = total.astype(BF16)
        tp_send(5, lambda t: final_ref.at[tp], final_ref.at[tp], recv8)

    got_trade(0)
    s1(0)
    project()
    s1(1)
    s2(0)
    share()
    s3(0)
    s1(2)
    queries()
    s2(1)
    scores()
    s4(0)
    values()
    s3(1)
    s2(2)
    over_tp()
    s5(0)
    s4(1)
    out_project(finish())
    s3(2)
    s4(2)
    reduce_out()
    s5(1)
    s5(2)
    tile = w_ref.at[5 - core]
    whole = remote(tile, tile, pair_sem.at[0], pair_sem.at[1], tp_peer(0, 1))
    whole.wait_send()
    whole.wait_recv()
    tp_wait(5, final_ref, recv8)
    for kind in range(3):
        sent = tiles_ref.at[0 : (14 if kind < 2 else 7)]
        remote(sent, sent, trade_send.at[kind], trade_recv.at[kind, 1], tp_peer(0, 1)).wait_send()
    across.wait_send()
    sent_all(0, r2, 15)
    sent_all(1, qb, 7)
    sent_all(2, ob, 7)
    sent_all(3, r6, 7)
    sent_all(4, po, 7)
    sent_all(5, final_ref, 7)


def layer(hidden, gain, bias, qkv_rows, out_rows, lengths, positions, keys, values):
    hbm, vmem = pl.BlockSpec(memory_space=pltpu.HBM), pl.BlockSpec(memory_space=pltpu.VMEM)
    smem, dma = pl.BlockSpec(memory_space=pltpu.SMEM), pltpu.SemaphoreType.DMA
    return pl.pallas_call(
        layer_kernel,
        name="layer",
        out_shape=(
            jax.ShapeDtypeStruct((6, 8, 8, 2, GROUPS, 4, HD), BF16),
            jax.ShapeDtypeStruct((4, 2 * KVH * HD), BF16),
            jax.ShapeDtypeStruct((8, 4, 512), BF16),
        ),
        in_specs=[hbm, hbm, hbm, hbm, hbm, smem, smem, hbm, hbm],
        out_specs=(vmem, vmem, vmem),
        scratch_shapes=[
            pltpu.VMEM((4, 3584), BF16),
            pltpu.VMEM((1, 3584), BF16),
            pltpu.VMEM((24, HD), BF16),
            pltpu.VMEM((ROWS, 24 * HD), BF16),
            pltpu.VMEM((ROWS, 16 * HD), BF16),
            pltpu.VMEM((40, GROUPS, 4, HD), BF16),
            pltpu.VMEM((8, 512), F32),
            pltpu.VMEM((24, HD), F32),
            pltpu.VMEM((3, 2, 4, HD), F32),
            pltpu.VMEM((4, HERE, KVH * HD), BF16),
            pltpu.VMEM((4, HERE, KVH * HD), BF16),
            pltpu.VMEM((2, 8, 8 * ROWS), BF16),
            pltpu.VMEM((8, 8 * ROWS), BF16),
            pltpu.VMEM((8 * ROWS, 3 * HD), BF16),
            pltpu.VMEM((2, 4, 3 * HD), F32),
            pltpu.VMEM((16, 4, 3 * HD), F32),
            pltpu.VMEM((8, 3, 4, HD), BF16),
            pltpu.VMEM((2, 64, HD), F32),
            pltpu.VMEM((64, HD), F32),
            pltpu.VMEM((64, HERE), F32),
            pltpu.VMEM((64, HERE), BF16),
            pltpu.VMEM((8, 3, 8, HD), F32),
            pltpu.VMEM((8, 3, 8, HD), F32),
            pltpu.VMEM((3, 8, HD), F32),
            pltpu.VMEM((8, 3, 8, HD), F32),
            pltpu.VMEM((8, 4, 512), F32),
            pltpu.VMEM((8, 4, 512), F32),
            dma((5,)), dma((2, 4)), dma((3,)), dma((3, 8)), dma((3,)), dma((3, 40)), dma((2,)), dma((2,)),
            dma((6,)), dma((16,)), dma((8,)), dma((8,)), dma((8,)), dma((8,)), dma((8,)),
        ],
        compiler_params=pltpu.CompilerParams(
            collective_id=0, has_side_effects=True, vmem_limit_bytes=40 * 2**20
        ),
    )(hidden, gain, bias, qkv_rows, out_rows, lengths, positions, keys, values)


def place_kernel(w_ref, fresh_ref, final_ref, attended_ref, fresh_out, qkv_ref, out_ref, sems):
    copies = []
    for k in range(6):
        target = out_ref.at[:, k * HD : (k + 1) * HD] if k < 2 else qkv_ref.at[:, (k - 2) * HD : (k - 1) * HD]
        copies.append(pltpu.make_async_copy(w_ref.at[k], target, sems.at[k]))
    for copy in copies:
        copy.start()
    fresh_out[...] = fresh_ref[...]
    for o in range(8):
        attended_ref[:, o * 448 : (o + 1) * 448] = final_ref[o, :, 0:448]
    for copy in copies:
        copy.wait()


def place(w, fresh, final):
    hbm, vmem = pl.BlockSpec(memory_space=pltpu.HBM), pl.BlockSpec(memory_space=pltpu.VMEM)
    return pl.pallas_call(
        place_kernel,
        name="place",
        out_shape=(
            jax.ShapeDtypeStruct((4, 3584), BF16),
            jax.ShapeDtypeStruct((4, 1024), BF16),
            jax.ShapeDtypeStruct((3584, 512), BF16),
            jax.ShapeDtypeStruct((3584, 256), BF16),
        ),
        in_specs=[vmem, vmem, vmem],
        out_specs=(vmem, vmem, hbm, hbm),
        scratch_shapes=[pltpu.SemaphoreType.DMA((6,))],
        compiler_params=pltpu.CompilerParams(vmem_limit_bytes=8 * 2**20),
    )(w, fresh, final)


def body(
    hidden,
    norm_gain,
    qkv_bias,
    qkv_weight,
    out_weight,
    key_cache,
    value_cache,
    cache_len,
    block_pos,
):
    fixed = (hidden, norm_gain.reshape(1, 3584), qkv_bias.reshape(24, HD), qkv_weight, out_weight)
    fixed = [pltpu.with_memory_space_constraint(a, pltpu.HBM) for a in fixed]
    caches = [pltpu.with_memory_space_constraint(a, pltpu.HBM) for a in (key_cache, value_cache)]
    w, fresh_kv, final = layer(*fixed, cache_len, block_pos, *caches)
    return place(w.reshape(6, 3584, HD), fresh_kv, final)


def solution(mesh):
    finer = Mesh(
        mesh.devices.reshape(2, 4, 4, 2, mesh.shape["roll"]),
        ("seq_0", "seq_1", "tp_0", "tp_1", "roll"),
    )
    in_specs = (
        P("roll", None),
        P(),
        P(),
        P(SEQ_TP_ROLL, None),
        P(SEQ_TP_ROLL, None),
        P("roll", SEQ_TP, None),
        P("roll", SEQ_TP, None),
        P("roll"),
        P("roll", SEQ_TP),
    )
    out_specs = (P("roll", None), P("roll", None), P(None, TP), P(None, TP))
    return jax.shard_map(body, mesh=finer, in_specs=in_specs, out_specs=out_specs, check_vma=False)
```

```python
import jax
import jax.numpy as jnp
import numpy as np
from jax import lax
from jax.experimental import pallas as pl
from jax.experimental.pallas import tpu as pltpu
from jax.sharding import Mesh
from jax.sharding import PartitionSpec as P

HQ = 16
KVH = 4
HD = 128
BLOCK = 512
STRETCH = 8192
ROWS = 28
PLACE = 4
GROUPS = 7
HERE = 1024
TP = ("tp_0", "tp_1")
SEQ = ("seq_0", "seq_1")
SEQ_TP = ("seq_0", "seq_1", "tp_0", "tp_1")
SEQ_TP_ROLL = ("seq_0", "seq_1", "tp_0", "tp_1", "roll")
MESH = pl.DeviceIdType.MESH
F32 = jnp.float32
BF16 = jnp.bfloat16

rope_base = 10000000.0
norm_eps = 1e-06
lowest = -1e30
floor_top = -1e20


def frequencies(width):
    half_width = width // 2
    exact = rope_base ** (-2.0 * np.arange(half_width) / width)
    octave = np.floor(np.log2(exact))
    quantum = 2.0 ** (8.0 - octave)
    return np.floor(exact * quantum) / quantum


def device(x, y, z, core):
    return (x % 2, z, y, core, x // 2)


ORDER = (0, -1, 1, 2)
TP_STEPS = tuple((dy, dc) for dy in (0, 3, 1, 2) for dc in (0, 1))
PLANE_STEPS = tuple((dx, dz) for dx in (2, 1, 3, 0) for dz in (2, 1, 3, 0))


STEPS = (
    ("ownA", 1), ("ownA", 0), ("ownB", 1), ("ownB", 2), ("ownB", 0), ("project",), ("f1m", 2, 1),
    ("f1m", 2, 0), ("f1p", 2, 1), ("f1m", 0, 0), ("f1m", 0, 1), ("f1p", 0, 0), ("share",), ("f1p", 0, 1),
    ("f2", 2, 1), ("f1p", 1, 1), ("gm", 0, 1, 0), ("f1m", 1, 0), ("gm", 0, 0, 0), ("f1p", 2, 0),
    ("gp", 0, 0, 1), ("f2", 0, 0), ("gp", 0, 0, 0), ("gp", 0, 1, 0), ("queries",), ("f1p", 1, 0),
    ("f2", 0, 1), ("scores",), ("gm", 0, 1, 1), ("gm", 0, 0, -1), ("gp", 0, 1, 1), ("values",),
    ("gp", 0, 1, -1), ("gp", 0, 0, -1), ("f1m", 1, 1), ("gm", 0, 1, -1), ("gp", 2, 1, -1), ("f2", 2, 0),
    ("gm", 0, 0, 2), ("gp", 0, 0, 2), ("gm", 0, 0, 1), ("gp", 0, 1, 2), ("gm", 0, 1, 2), ("gm", 2, 1, 0),
    ("gm", 2, 0, 1), ("over_tp",), ("f2", 1, 0), ("gp", 2, 0, 1), ("f2", 1, 1), ("gm", 2, 1, 1),
    ("gp", 1, 0, 1), ("gp", 2, 1, 1), ("gm", 1, 1, -1), ("gm", 1, 0, 1), ("gp", 1, 1, 0), ("gm", 1, 0, 0),
    ("gm", 2, 0, 0), ("gp", 2, 0, 2), ("gp", 1, 1, 1), ("gm", 2, 1, -1), ("gp", 2, 1, 2), ("gm", 1, 1, 1),
    ("gp", 1, 0, 0), ("gp", 2, 0, 0), ("gm", 1, 1, 0), ("gm", 1, 0, -1), ("gm", 2, 0, 2), ("gp", 1, 0, -1),
    ("stage_out",), ("out_project",), ("gm", 2, 1, 2), ("gp", 2, 1, 0), ("gp", 1, 1, -1), ("gm", 2, 0, -1),
    ("gp", 2, 0, -1), ("gp", 1, 0, 2), ("gp", 1, 1, 2), ("gm", 1, 1, 2), ("gm", 1, 0, 2), ("reduce_out",),
)


def layer_kernel(
    hidden_ref, gain_ref, bias_hbm, qkv_ref, out_ref, len_ref, pos_ref, key_ref, value_ref,
    w_ref, fresh_ref, final_ref,
    len_smem, pos_smem, hidden_in, gain_in, gain_row, bias_in, qkv_in, out_in, tiles_ref, near, bias_ref, turn_ref,
    kbuf, vbuf, normed_ref, other, wo, wq, part, r2, qb, rot, self_s, s_buf, p_buf, ob, r5, c6, r6, po, r7,
    line_sem, load_sem, cache_sem, trade_send, trade_recv, ring_send, ring_recv, pair_sem, other_sem,
    stage_send, recv2, recv3, recv5, recv6, recv7, recv8,
):
    x = lax.axis_index("roll") * 2 + lax.axis_index("seq_0")
    y, z, core = lax.axis_index("tp_0"), lax.axis_index("seq_1"), lax.axis_index("tp_1")
    seq, roll, tp = (x % 2) * 4 + z, x // 2, y * 2 + core

    def remote(src, dst, send, recv, target):
        return pltpu.make_async_remote_copy(
            src_ref=src, dst_ref=dst, send_sem=send, recv_sem=recv,
            device_id=device(*target), device_id_type=MESH,
        )

    def tp_peer(dy, dc):
        return (x, (y + dy) % 4, z, (core + dc) % 2)

    def plane_peer(dx, dz):
        return ((x + dx) % 4, y, (z + dz) % 4, core)

    partners = [tp_peer(dy, dc) for dy, dc in TP_STEPS if (dy, dc) != (0, 0)]
    partners += [plane_peer(dx, dz) for dx, dz in PLANE_STEPS if (dx == 0) != (dz == 0)]

    caches = []
    for r in range(4):
        caches.append(pltpu.make_async_copy(key_ref.at[r], kbuf.at[r], cache_sem.at[0, r]))
    for r in range(4):
        caches.append(pltpu.make_async_copy(value_ref.at[r], vbuf.at[r], cache_sem.at[1, r]))

    barrier = pltpu.get_barrier_semaphore()
    for partner in partners:
        pl.semaphore_signal(barrier, inc=1, device_id=device(*partner), device_id_type=MESH)
    loads = [
        pltpu.make_async_copy(src, dst, load_sem.at[k])
        for k, (src, dst) in enumerate((
            (out_ref, out_in), (qkv_ref, qkv_in), (hidden_ref, hidden_in), (gain_ref, gain_in), (bias_hbm, bias_in),
            (len_ref, len_smem), (pos_ref, pos_smem),
        ))
    ]
    for copy in loads:
        copy.start()

    def stage(source, first, count):
        for k in range(count):
            tiles_ref[first + k] = source[:, k * HD : (k + 1) * HD].reshape(GROUPS, 4, HD)

    def select_rows():
        wide = hidden_in[...].astype(F32)
        scale = lax.rsqrt(jnp.sum(wide * wide, axis=1, keepdims=True) * (1.0 / 3584) + norm_eps)
        gain_row[...] = gain_in[...].astype(F32).reshape(1, 3584)
        base = pl.multiple_of(((7 * seq) // 2) * HD, HD)
        wide = hidden_in[:, pl.ds(base, 512)].astype(F32) * scale * gain_row[:, pl.ds(base, 512)]
        near[0:4] = wide
        near[4:8] = jnp.zeros((4, 512), F32)
        lhs = near[...].astype(BF16)
        feature = lax.broadcasted_iota(jnp.int32, (512, 8 * ROWS), 0) + (base - seq * 448)
        column = lax.broadcasted_iota(jnp.int32, (512, 8 * ROWS), 1)
        wanted = column + (column // ROWS) * ROWS
        for k, r in ((0, roll), (1, 1 - roll)):
            picked = jnp.where(feature == wanted + r * ROWS, 1.0, 0.0).astype(BF16)
            normed_ref[k] = jnp.dot(lhs, picked, preferred_element_type=F32).astype(BF16)

    def tables():
        lane = lax.broadcasted_iota(jnp.int32, (4, HD), 1)
        row = lax.broadcasted_iota(jnp.int32, (4, HD), 0)
        freq = jnp.zeros((4, HD), F32)
        for k, value in enumerate(frequencies(HD)):
            freq = jnp.where(lane % 64 == k, jnp.float32(value), freq)
        for k in range(3):
            position = jnp.zeros((4, HD), jnp.int32)
            for r in range(4):
                here = len_smem[r] % STRETCH if k == 0 else pos_smem[k - 1, r]
                position = jnp.where(row == r, here, position)
            angle = position.astype(F32) * freq
            turn_ref[k, 0] = jnp.cos(angle)
            sine = jnp.sin(angle)
            turn_ref[k, 1] = jnp.where(lane < 64, -sine, sine)

    def tiles_of(kind, ty, tcore):
        t = ty * 2 + tcore
        return (24 + 2 * t, 2) if kind == 0 else (2 * t, 2) if kind == 1 else (16 + 4 * tcore + ty, 1)

    def place_of(kind, tcore):
        return (0, 2) if kind == 0 else (2, 2) if kind == 1 else (4 + tcore, 1)

    def traded(kind, dy, dc):
        ty, tcore = (y + dy) % 4, (core + dc) % 2
        first, count = tiles_of(kind, ty, tcore)
        to, _ = place_of(kind, tcore)
        src = tiles_ref.at[pl.ds(first, count)]
        dst = w_ref.at[pl.ds(to, count), seq, tp, roll]
        return remote(src, dst, trade_send.at[kind], trade_recv.at[kind, dy * 2 + dc], (x, ty, z, tcore))

    def got_trade(kind, steps):
        to, count = place_of(kind, core)
        for dy, dc in steps:
            if (dy, dc) != (0, 0):
                source = ((y - dy) % 4) * 2 + (core + dc) % 2
                here = w_ref.at[pl.ds(to, count), seq, source, roll]
                remote(here, here, trade_send.at[kind], trade_recv.at[kind, dy * 2 + dc], tp_peer(dy, dc)).wait_recv()

    def keep_own(kind):
        first, count = tiles_of(kind, y, core)
        to, _ = place_of(kind, core)
        for k in range(count):
            w_ref[to + k, seq, tp, roll] = tiles_ref[first + k]

    loads[0].wait()
    stage(out_in, 24, 16)
    keep_own(0)
    loads[1].wait()
    stage(qkv_in, 0, 24)
    keep_own(1)
    keep_own(2)
    for k in range(2, 7):
        loads[k].wait()
    select_rows()
    pl.semaphore_wait(barrier, len(partners))
    for dx in (1, 2, 3):
        pl.semaphore_signal(line_sem, inc=1, device_id=device(*plane_peer(dx, 0)), device_id_type=MESH)

    for kind in (1, 2, 0):
        traded(kind, 0, 1).start()
    across = remote(normed_ref.at[1], other, other_sem.at[0], other_sem.at[1], plane_peer(2, 0))
    across.start()
    for kind in (1, 2, 0):
        for dy, dc in TP_STEPS:
            if dy != 0:
                traded(kind, dy, dc).start()
    for copy in caches:
        copy.start()
    tables()
    bias_ref[...] = bias_in[...].astype(F32)

    def region(kind, half):
        if kind < 2:
            return kind * 2 + half, 0, 8
        return 4 + core, half * 4, 4

    def block_at(kind, half, bx, bz, part_of):
        tile, first, count = region(kind, half)
        if part_of is not None:
            count = count // 2
            first = first + part_of * count
        return w_ref.at[pl.ds(tile, 1), (bx % 2) * 4 + bz, pl.ds(first, count), bx // 2]

    def coords(half, f, g):
        return ((x + g) % 4, (z + f) % 4) if half == 0 else ((x + f) % 4, (z + g) % 4)

    def ring(kind, half, message, f, g, part_of, step):
        bx, bz = coords(half, f, g)
        tx, tz = coords(half, *step)
        block = block_at(kind, half, bx, bz, part_of)
        return remote(block, block, ring_send.at[kind], ring_recv.at[kind, half * 20 + message], (tx, y, tz, core))

    def to_pair(kind, half, f, g, part_of=None):
        if kind == 2:
            bx, bz = coords(half, f, g)
            block = block_at(kind, half, bx, bz, part_of)
            remote(block, block, pair_sem.at[0], pair_sem.at[1], tp_peer(0, 1)).start()

    def sideways(kind, half, f):
        k = 4 + ORDER.index(f) * 4
        ring(kind, half, k, f, 0, None, (0, 1)).start()
        ring(kind, half, k + 1, f, 0, None, (0, -1)).start()

    def own_rows(kind, dys):
        for message, along in ((0, (1, 0)), (1, (-1, 0)), (4, (0, 1)), (5, (0, -1))):
            for half in (0, 1):
                tx, tz = coords(half, *along)
                tile, _, _ = region(kind, half)
                for dy in dys:
                    first = ((y - dy) % 4) * 2
                    block = w_ref.at[pl.ds(tile, 1), seq, pl.ds(first, 2), roll]
                    if kind == 2:
                        continue
                    remote(
                        block, block, ring_send.at[kind], ring_recv.at[kind, half * 20 + message], (tx, y, tz, core)
                    ).start()
                if kind == 2 and 0 not in dys:
                    block = block_at(kind, half, x, z, None)
                    remote(
                        block, block, ring_send.at[kind], ring_recv.at[kind, half * 20 + message], (tx, y, tz, core)
                    ).start()
        if kind == 2 and 0 not in dys:
            for half in (0, 1):
                to_pair(kind, half, 0, 0)

    def first_step(kind, half, f):
        ring(kind, half, 0 if f < 0 else 1, f, 0, None, (1, 0)).wait_recv()
        if f < 0:
            ring(kind, half, 2, f, 0, 0, (1, 0)).start()
        else:
            ring(kind, half, 3, f, 0, 1, (-1, 0)).start()
        sideways(kind, half, f)
        to_pair(kind, half, f, 0)

    def far_step(kind, half):
        ring(kind, half, 2, 2, 0, 0, (1, 0)).wait_recv()
        ring(kind, half, 3, 2, 0, 1, (1, 0)).wait_recv()
        sideways(kind, half, 2)
        to_pair(kind, half, 2, 0)

    def side_step(kind, half, f, g):
        k = 4 + ORDER.index(f) * 4
        if g < 0:
            ring(kind, half, k, f, -1, None, (0, 1)).wait_recv()
            ring(kind, half, k + 2, f, -1, 0, (0, 1)).start()
        else:
            ring(kind, half, k + 1, f, 1, None, (0, 1)).wait_recv()
            ring(kind, half, k + 3, f, 1, 1, (0, -1)).start()
        to_pair(kind, half, f, g)

    def last_step(kind):
        for f in ORDER:
            for half in (0, 1):
                k = 4 + ORDER.index(f) * 4
                ring(kind, half, k + 2, f, 2, 0, (0, 1)).wait_recv()
                to_pair(kind, half, f, 2, 0)
                ring(kind, half, k + 3, f, 2, 1, (0, 1)).wait_recv()
                to_pair(kind, half, f, 2, 1)

    def sent_ring(kind):
        sent = w_ref.at[0:5, 0 : (6 if kind < 2 else 3), :, 0]
        remote(sent, sent, ring_send.at[kind], ring_recv.at[kind, 0], plane_peer(0, 1)).wait_send()

    def tp_send(stage, src_of, dst, sems):
        for dy, dc in TP_STEPS:
            if (dy, dc) != (0, 0):
                target = tp_peer(dy, dc)
                remote(src_of(target[1] * 2 + target[3]), dst, stage_send.at[stage], sems.at[dy * 2 + dc], target).start()

    def tp_wait(stage, buffer, sems):
        for dy, dc in TP_STEPS:
            if (dy, dc) != (0, 0):
                here = buffer.at[((y - dy) % 4) * 2 + (core + dc) % 2]
                remote(here, here, stage_send.at[stage], sems.at[dy * 2 + dc], tp_peer(dy, dc)).wait_recv()

    def sent_all(stage, buffer, count):
        sent = buffer.at[0:count]
        remote(sent, sent, stage_send.at[stage], recv3.at[0], tp_peer(0, 1)).wait_send()

    def project():
        across.wait_recv()
        for k in range(3):
            tile = (2 + k) if k < 2 else 4 + core
            rows = w_ref[tile, seq, :, roll]
            wq[:, k * HD : (k + 1) * HD] = rows.reshape(8 * ROWS, HD)
        for k, lhs in ((0, normed_ref[0]), (1, other[...])):
            made = jnp.dot(lhs, wq[...], preferred_element_type=F32)
            part[k] = made[0:4]
        r2[x * 4 + z] = part[0]
        pl.semaphore_wait(line_sem, 3)
        for dx, dz in PLANE_STEPS:
            if (dx, dz) != (0, 0):
                tx, _, tz, _ = plane_peer(dx, dz)
                remote(
                    part.at[(tx // 2 + roll) % 2], r2.at[x * 4 + z], stage_send.at[0],
                    recv2.at[dx * 4 + dz], (tx, y, tz, core),
                ).start()

    def share():
        for dx, dz in PLANE_STEPS:
            if (dx, dz) != (0, 0):
                here = r2.at[((x - dx) % 4) * 4 + (z - dz) % 4]
                remote(here, here, stage_send.at[0], recv2.at[dx * 4 + dz], plane_peer(dx, dz)).wait_recv()
        total = r2[0]
        for k in range(1, 16):
            total = total + r2[k]
        for k in range(3):
            row = (2 * tp + k) if k < 2 else 16 + 4 * core + y
            qb[tp, k] = (total[:, k * HD : (k + 1) * HD] + bias_ref[pl.ds(row, 1)]).astype(BF16)
        tp_send(1, lambda t: qb.at[tp], qb.at[tp], recv3)

    def turn(v, position):
        return v * turn_ref[position, 0] + pltpu.roll(v, 64, v.ndim - 1) * turn_ref[position, 1]

    def queries():
        tp_wait(1, qb, recv3)
        for g in range(KVH):
            fresh_key = turn(qb[2 * g, 2].astype(F32), 0).astype(BF16)
            fresh_ref[:, g * HD : (g + 1) * HD] = fresh_key
            fresh_ref[:, (KVH + g) * HD : (KVH + g + 1) * HD] = qb[2 * g + 1, 2]
            for h in range(4 * g, 4 * g + 4):
                q = qb[h // 2, h % 2].astype(F32)
                own = turn(q, 0).astype(BF16).astype(F32)
                score = jnp.sum(own * fresh_key.astype(F32), axis=1, keepdims=True) * HD ** (-0.5)
                self_s[4 * h : 4 * h + 4] = jnp.broadcast_to(score, (4, HD))
                for b in range(2):
                    rot[b, 4 * h : 4 * h + 4] = turn(q, 1 + b)

    def scores():
        start = (seq * 8 + tp) * HERE
        owner = lax.broadcasted_iota(jnp.int32, (16, BLOCK), 0) % 4
        column = lax.broadcasted_iota(jnp.int32, (16, BLOCK), 1)
        for r in range(4):
            caches[r].wait()
            for b in range(2):
                valid = (owner == r) & (column + (start + b * BLOCK) < len_smem[r])
                for g in range(KVH):
                    rows, cols = slice(16 * g, 16 * g + 16), slice(b * BLOCK, (b + 1) * BLOCK)
                    made = lax.dot_general(
                        rot[b, rows].astype(BF16), kbuf[r, cols, g * HD : (g + 1) * HD],
                        (((1,), (1,)), ((), ())), preferred_element_type=F32,
                    )
                    before = s_buf[rows, cols] if r > 0 else jnp.full((16, BLOCK), lowest, F32)
                    s_buf[rows, cols] = jnp.where(valid, made * HD ** (-0.5), before)

    def values():
        for g in range(KVH):
            s = s_buf[16 * g : 16 * g + 16]
            top = jnp.maximum(jnp.max(s, axis=1, keepdims=True), floor_top)
            w = jnp.exp(s - top)
            p_buf[16 * g : 16 * g + 16] = w.astype(BF16)
            low = jnp.sum(w, axis=1, keepdims=True)
            for k in range(2):
                rows = slice(8 * k, 8 * k + 8)
                ob[2 * g + k, 0] = jnp.broadcast_to(top[rows], (8, HD))
                ob[2 * g + k, 1] = jnp.broadcast_to(low[rows], (8, HD))
        owner = lax.broadcasted_iota(jnp.int32, (16, HERE), 0) % 4
        for r in range(4):
            caches[4 + r].wait()
        for g in range(KVH):
            total = jnp.zeros((16, HD), F32)
            w = p_buf[16 * g : 16 * g + 16].astype(F32)
            for r in range(4):
                mine = jnp.where(owner == r, w, 0.0).astype(BF16)
                total += jnp.dot(mine, vbuf[r, :, g * HD : (g + 1) * HD], preferred_element_type=F32)
            ob[2 * g, 2] = total[0:8]
            ob[2 * g + 1, 2] = total[8:16]
        r5[tp] = ob[tp]
        tp_send(2, lambda t: ob.at[t], r5.at[tp], recv5)

    def combined(buffer):
        top = buffer[0, 0]
        for k in range(1, 8):
            top = jnp.maximum(top, buffer[k, 0])
        low, out = jnp.zeros_like(top), jnp.zeros_like(top)
        for k in range(8):
            factor = jnp.exp(buffer[k, 0] - top)
            low += buffer[k, 1] * factor
            out += buffer[k, 2] * factor
        return top, low, out

    def over_tp():
        tp_wait(2, r5, recv5)
        for k, value in enumerate(combined(r5)):
            c6[k] = value
            r6[seq, k] = value
        for dl in range(2):
            for dz in (2, 1, 3, 0):
                if dl + dz > 0:
                    tx, tz = roll * 2 + (x + dl) % 2, (z + dz) % 4
                    remote(c6, r6.at[seq], stage_send.at[3], recv6.at[dl * 4 + dz], (tx, y, tz, core)).start()

    def finish():
        for dl in range(2):
            for dz in (2, 1, 3, 0):
                if dl + dz > 0:
                    here = r6.at[((x + dl) % 2) * 4 + (z - dz) % 4]
                    remote(here, here, stage_send.at[3], recv6.at[dl * 4 + dz], plane_peer(0, 1)).wait_recv()
        old_top, old_low, old_out = combined(r6)
        mine = self_s[pl.ds(pl.multiple_of(tp * 8, 8), 8)]
        top = jnp.maximum(old_top, mine)
        factor, fresh = jnp.exp(old_top - top), jnp.exp(mine - top)
        own_value = qb[(tp // 2) * 2 + 1, 2].astype(F32)
        both = jnp.concatenate([own_value, own_value], axis=0)
        numerator = old_out * factor + fresh.astype(BF16).astype(F32) * both
        attention = (numerator / (old_low * factor + fresh)).astype(BF16)
        return attention

    def stage_out():
        for o in range(8):
            for k in range(2):
                wo[k, o] = w_ref[k, o].reshape(16 * ROWS, HD)

    def out_project(attention):
        for o in range(8):
            sums = []
            for k in range(2):
                sums.append(lax.dot_general(attention, wo[k, o], (((1,), (1,)), ((), ())), preferred_element_type=F32))
            po[o, :, 0:448] = sums[0][0:4] + sums[1][4:8]
            po[o, :, 448:512] = jnp.zeros((4, 64), F32)
        r7[tp] = po[tp]
        tp_send(4, lambda t: po.at[t], r7.at[tp], recv7)

    def reduce_out():
        tp_wait(4, r7, recv7)
        total = r7[0]
        for k in range(1, 8):
            total = total + r7[k]
        final_ref[tp] = total.astype(BF16)
        tp_send(5, lambda t: final_ref.at[tp], final_ref.at[tp], recv8)

    pair, rest = ((0, 1),), tuple((dy, dc) for dy, dc in TP_STEPS if dy)
    had = set()

    def need(kind, *parts):
        for name, steps in (("pair", pair), ("rest", rest)):
            if name in parts and (kind, name) not in had:
                had.add((kind, name))
                got_trade(kind, steps)

    for name, *at in STEPS:
        if name == "ownA":
            need(at[0], "pair")
            own_rows(at[0], (0,))
        elif name == "ownB":
            need(at[0], "pair", "rest")
            own_rows(at[0], (3, 1, 2))
        elif name == "f1p":
            first_step(*at, -1)
        elif name == "f1m":
            first_step(*at, 1)
        elif name == "f2":
            far_step(*at)
        elif name == "gp":
            side_step(*at, -1)
        elif name == "gm":
            side_step(*at, 1)
        elif name == "project":
            need(1, "pair", "rest")
            need(2, "pair", "rest")
            project()
        elif name == "share":
            share()
        elif name == "queries":
            queries()
        elif name == "scores":
            scores()
        elif name == "values":
            values()
        elif name == "over_tp":
            over_tp()
        elif name == "stage_out":
            last_step(0)
            stage_out()
        elif name == "out_project":
            out_project(finish())
        elif name == "reduce_out":
            reduce_out()
    last_step(1)
    last_step(2)
    for kind in range(3):
        sent_ring(kind)
    tile = w_ref.at[5 - core]
    whole = remote(tile, tile, pair_sem.at[0], pair_sem.at[1], tp_peer(0, 1))
    whole.wait_send()
    whole.wait_recv()
    tp_wait(5, final_ref, recv8)
    for kind in range(3):
        sent = tiles_ref.at[0 : (14 if kind < 2 else 7)]
        remote(sent, sent, trade_send.at[kind], trade_recv.at[kind, 1], tp_peer(0, 1)).wait_send()
    across.wait_send()
    sent_all(0, r2, 15)
    sent_all(1, qb, 7)
    sent_all(2, ob, 7)
    sent_all(3, r6, 7)
    sent_all(4, po, 7)
    sent_all(5, final_ref, 7)


def layer(hidden, gain, bias, qkv_rows, out_rows, lengths, positions, keys, values):
    hbm, vmem = pl.BlockSpec(memory_space=pltpu.HBM), pl.BlockSpec(memory_space=pltpu.VMEM)
    dma = pltpu.SemaphoreType.DMA
    return pl.pallas_call(
        layer_kernel,
        name="layer",
        out_shape=(
            jax.ShapeDtypeStruct((6, 8, 8, 2, GROUPS, 4, HD), BF16),
            jax.ShapeDtypeStruct((4, 2 * KVH * HD), BF16),
            jax.ShapeDtypeStruct((8, 4, 512), BF16),
        ),
        in_specs=[hbm] * 9,
        out_specs=(vmem, vmem, vmem),
        scratch_shapes=[
            pltpu.SMEM((4,), jnp.int32),
            pltpu.SMEM((2, 4), jnp.int32),
            pltpu.VMEM((4, 3584), BF16),
            pltpu.VMEM((3584,), BF16),
            pltpu.VMEM((1, 3584), F32),
            pltpu.VMEM((24, HD), BF16),
            pltpu.VMEM((ROWS, 24 * HD), BF16),
            pltpu.VMEM((ROWS, 16 * HD), BF16),
            pltpu.VMEM((40, GROUPS, 4, HD), BF16),
            pltpu.VMEM((8, 512), F32),
            pltpu.VMEM((24, HD), F32),
            pltpu.VMEM((3, 2, 4, HD), F32),
            pltpu.VMEM((4, HERE, KVH * HD), BF16),
            pltpu.VMEM((4, HERE, KVH * HD), BF16),
            pltpu.VMEM((2, 8, 8 * ROWS), BF16),
            pltpu.VMEM((8, 8 * ROWS), BF16),
            pltpu.VMEM((2, 8, 16 * ROWS, HD), BF16),
            pltpu.VMEM((8 * ROWS, 3 * HD), BF16),
            pltpu.VMEM((2, 4, 3 * HD), F32),
            pltpu.VMEM((16, 4, 3 * HD), F32),
            pltpu.VMEM((8, 3, 4, HD), BF16),
            pltpu.VMEM((2, 64, HD), F32),
            pltpu.VMEM((64, HD), F32),
            pltpu.VMEM((64, HERE), F32),
            pltpu.VMEM((64, HERE), BF16),
            pltpu.VMEM((8, 3, 8, HD), F32),
            pltpu.VMEM((8, 3, 8, HD), F32),
            pltpu.VMEM((3, 8, HD), F32),
            pltpu.VMEM((8, 3, 8, HD), F32),
            pltpu.VMEM((8, 4, 512), F32),
            pltpu.VMEM((8, 4, 512), F32),
            pltpu.SemaphoreType.REGULAR, dma((7,)), dma((2, 4)), dma((3,)), dma((3, 8)), dma((3,)), dma((3, 40)), dma((2,)), dma((2,)),
            dma((6,)), dma((16,)), dma((8,)), dma((8,)), dma((8,)), dma((8,)), dma((8,)),
        ],
        compiler_params=pltpu.CompilerParams(
            collective_id=0, has_side_effects=True, vmem_limit_bytes=40 * 2**20
        ),
    )(hidden, gain, bias, qkv_rows, out_rows, lengths, positions, keys, values)


def place_kernel(w_ref, fresh_ref, final_ref, attended_ref, fresh_out, qkv_ref, out_ref, sems):
    copies = []
    for k in range(6):
        target = out_ref.at[:, k * HD : (k + 1) * HD] if k < 2 else qkv_ref.at[:, (k - 2) * HD : (k - 1) * HD]
        for part in range(PLACE):
            rows = slice(part * 3584 // PLACE, (part + 1) * 3584 // PLACE)
            copies.append(pltpu.make_async_copy(w_ref.at[k, rows], target.at[rows], sems.at[k, part]))
    for copy in copies:
        copy.start()
    fresh_out[...] = fresh_ref[...]
    for o in range(8):
        attended_ref[:, o * 448 : (o + 1) * 448] = final_ref[o, :, 0:448]
    for copy in copies:
        copy.wait()


def place(w, fresh, final):
    hbm, vmem = pl.BlockSpec(memory_space=pltpu.HBM), pl.BlockSpec(memory_space=pltpu.VMEM)
    return pl.pallas_call(
        place_kernel,
        name="place",
        out_shape=(
            jax.ShapeDtypeStruct((4, 3584), BF16),
            jax.ShapeDtypeStruct((4, 1024), BF16),
            jax.ShapeDtypeStruct((3584, 512), BF16),
            jax.ShapeDtypeStruct((3584, 256), BF16),
        ),
        in_specs=[vmem, vmem, vmem],
        out_specs=(vmem, vmem, hbm, hbm),
        scratch_shapes=[pltpu.SemaphoreType.DMA((6, PLACE))],
        compiler_params=pltpu.CompilerParams(vmem_limit_bytes=8 * 2**20),
    )(w, fresh, final)


def body(
    hidden,
    norm_gain,
    qkv_bias,
    qkv_weight,
    out_weight,
    key_cache,
    value_cache,
    cache_len,
    block_pos,
):
    operands = (
        hidden, norm_gain, qkv_bias.reshape(24, HD), qkv_weight, out_weight,
        cache_len, block_pos.T, key_cache, value_cache,
    )
    w, fresh_kv, final = layer(*(pltpu.with_memory_space_constraint(a, pltpu.HBM) for a in operands))
    return place(w.reshape(6, 3584, HD), fresh_kv, final)


def solution(mesh):
    finer = Mesh(
        mesh.devices.reshape(2, 4, 4, 2, mesh.shape["roll"]),
        ("seq_0", "seq_1", "tp_0", "tp_1", "roll"),
    )
    in_specs = (
        P("roll", None),
        P(),
        P(),
        P(SEQ_TP_ROLL, None),
        P(SEQ_TP_ROLL, None),
        P("roll", SEQ_TP, None),
        P("roll", SEQ_TP, None),
        P("roll"),
        P("roll", SEQ_TP),
    )
    out_specs = (P("roll", None), P("roll", None), P(None, TP), P(None, TP))
    return jax.shard_map(body, mesh=finer, in_specs=in_specs, out_specs=out_specs, check_vma=False)
```

```python
import jax
import jax.numpy as jnp
import numpy as np
from jax import lax
from jax.experimental import pallas as pl
from jax.experimental.pallas import tpu as pltpu
from jax.sharding import Mesh
from jax.sharding import PartitionSpec as P

HQ = 16
KVH = 4
HD = 128
BLOCK = 512
STRETCH = 8192
ROWS = 28
PLACE = 4
GROUPS = 7
HERE = 1024
TP = ("tp_0", "tp_1")
SEQ = ("seq_0", "seq_1")
SEQ_TP = ("seq_0", "seq_1", "tp_0", "tp_1")
SEQ_TP_ROLL = ("seq_0", "seq_1", "tp_0", "tp_1", "roll")
MESH = pl.DeviceIdType.MESH
F32 = jnp.float32
BF16 = jnp.bfloat16

rope_base = 10000000.0
norm_eps = 1e-06
lowest = -1e30
floor_top = -1e20


def frequencies(width):
    half_width = width // 2
    exact = rope_base ** (-2.0 * np.arange(half_width) / width)
    octave = np.floor(np.log2(exact))
    quantum = 2.0 ** (8.0 - octave)
    return np.floor(exact * quantum) / quantum


def device(x, y, z, core):
    return (x % 2, z, y, core, x // 2)


ORDER = (0, -1, 1, 2)
TP_STEPS = tuple((dy, dc) for dy in (0, 3, 1, 2) for dc in (0, 1))
PLANE_STEPS = tuple((dx, dz) for dx in (2, 1, 3, 0) for dz in (2, 1, 3, 0))


STEPS = (
    ("ownA", 1), ("ownA", 0), ("ownB", 1), ("ownB", 2), ("ownB", 0), ("project",), ("gp", 2, 0, 0),
    ("f1m", 0, 1), ("f1p", 0, 0), ("f1p", 0, 1), ("gm", 1, 0, 0), ("gp", 0, 1, 0), ("gp", 2, 1, 0),
    ("f1m", 0, 0), ("f1m", 2, 0), ("f1p", 1, 1), ("share",), ("f1m", 1, 1), ("f1p", 2, 0), ("f2", 0, 1),
    ("f1m", 1, 0), ("f1p", 2, 1), ("gp", 0, 1, -1), ("f1m", 2, 1), ("gm", 0, 1, 0), ("f2", 0, 0),
    ("gm", 0, 0, 1), ("f1p", 1, 0), ("gm", 0, 1, -1), ("gp", 0, 1, 1), ("gp", 0, 0, -1), ("gm", 2, 0, 0),
    ("queries",), ("scores",), ("values",), ("gm", 0, 0, 0), ("gm", 0, 0, -1), ("f2", 1, 1), ("gp", 2, 0, -1),
    ("f2", 2, 0), ("gp", 0, 0, 2), ("gm", 0, 1, 2), ("gp", 0, 0, 0), ("gp", 0, 1, 2), ("f2", 2, 1),
    ("gm", 0, 0, 2), ("gp", 0, 0, 1), ("gm", 0, 1, 1), ("over_tp",), ("f2", 1, 0), ("gp", 2, 1, 1),
    ("gm", 2, 0, -1), ("gm", 1, 1, 1), ("gm", 1, 1, 2), ("gp", 2, 1, -1), ("gp", 2, 0, 2), ("gp", 1, 0, 0),
    ("gp", 1, 1, 1), ("gm", 1, 1, -1), ("gm", 2, 1, 0), ("gp", 1, 0, 1), ("gm", 2, 1, 1), ("gm", 2, 0, 2),
    ("gp", 1, 1, 0), ("gm", 1, 0, -1), ("gm", 2, 1, -1), ("gp", 1, 0, -1), ("gp", 1, 1, -1), ("stage_out",),
    ("out_project",), ("gm", 2, 0, 1), ("gp", 2, 0, 1), ("gm", 1, 1, 0), ("gp", 2, 1, 2), ("gm", 1, 0, 1),
    ("gp", 1, 1, 2), ("gm", 2, 1, 2), ("gp", 1, 0, 2), ("gm", 1, 0, 2), ("reduce_out",),
)


def layer_kernel(
    hidden_ref, gain_ref, bias_hbm, qkv_ref, out_ref, len_ref, pos_ref, key_ref, value_ref,
    w_ref, fresh_ref, final_ref,
    len_smem, pos_smem, hidden_in, gain_in, gain_row, bias_in, qkv_in, out_in, tiles_ref, near, bias_ref, turn_ref,
    kbuf, vbuf, normed_ref, other, wo, wq, part, r2, qb, rot, self_s, s_buf, p_buf, ob, r5, c6, r6, po, r7,
    line_sem, load_sem, cache_sem, trade_send, trade_recv, ring_send, ring_recv, pair_sem, other_sem,
    stage_send, recv2, recv3, recv5, recv6, recv7, recv8,
):
    x = lax.axis_index("roll") * 2 + lax.axis_index("seq_0")
    y, z, core = lax.axis_index("tp_0"), lax.axis_index("seq_1"), lax.axis_index("tp_1")
    seq, roll, tp = (x % 2) * 4 + z, x // 2, y * 2 + core

    def remote(src, dst, send, recv, target):
        return pltpu.make_async_remote_copy(
            src_ref=src, dst_ref=dst, send_sem=send, recv_sem=recv,
            device_id=device(*target), device_id_type=MESH,
        )

    def tp_peer(dy, dc):
        return (x, (y + dy) % 4, z, (core + dc) % 2)

    def plane_peer(dx, dz):
        return ((x + dx) % 4, y, (z + dz) % 4, core)

    partners = [tp_peer(dy, dc) for dy, dc in TP_STEPS if (dy, dc) != (0, 0)]
    partners += [plane_peer(dx, dz) for dx, dz in PLANE_STEPS if (dx == 0) != (dz == 0)]

    caches = []
    for r in range(4):
        caches.append(pltpu.make_async_copy(key_ref.at[r], kbuf.at[r], cache_sem.at[0, r]))
    for r in range(4):
        caches.append(pltpu.make_async_copy(value_ref.at[r], vbuf.at[r], cache_sem.at[1, r]))

    barrier = pltpu.get_barrier_semaphore()
    for partner in partners:
        pl.semaphore_signal(barrier, inc=1, device_id=device(*partner), device_id_type=MESH)
    loads = [
        pltpu.make_async_copy(src, dst, load_sem.at[k])
        for k, (src, dst) in enumerate((
            (qkv_ref, qkv_in), (out_ref, out_in), (hidden_ref, hidden_in), (gain_ref, gain_in), (bias_hbm, bias_in),
            (len_ref, len_smem), (pos_ref, pos_smem),
        ))
    ]
    for copy in loads + caches:
        copy.start()

    def stage(source, first, count):
        start = first % 24
        for k in range(start, start + count):
            tiles_ref[first + k - start] = source[:, k * HD : (k + 1) * HD].reshape(GROUPS, 4, HD)

    def select_rows():
        wide = hidden_in[...].astype(F32)
        scale = lax.rsqrt(jnp.sum(wide * wide, axis=1, keepdims=True) * (1.0 / 3584) + norm_eps)
        gain_row[...] = gain_in[...].astype(F32).reshape(1, 3584)
        base = pl.multiple_of(((7 * seq) // 2) * HD, HD)
        wide = hidden_in[:, pl.ds(base, 512)].astype(F32) * scale * gain_row[:, pl.ds(base, 512)]
        near[0:4] = wide
        near[4:8] = jnp.zeros((4, 512), F32)
        lhs = near[...].astype(BF16)
        feature = lax.broadcasted_iota(jnp.int32, (512, 8 * ROWS), 0) + (base - seq * 448)
        column = lax.broadcasted_iota(jnp.int32, (512, 8 * ROWS), 1)
        wanted = column + (column // ROWS) * ROWS
        for k, r in ((0, roll), (1, 1 - roll)):
            picked = jnp.where(feature == wanted + r * ROWS, 1.0, 0.0).astype(BF16)
            normed_ref[k] = jnp.dot(lhs, picked, preferred_element_type=F32).astype(BF16)

    def tables():
        lane = lax.broadcasted_iota(jnp.int32, (4, HD), 1)
        row = lax.broadcasted_iota(jnp.int32, (4, HD), 0)
        freq = jnp.zeros((4, HD), F32)
        for k, value in enumerate(frequencies(HD)):
            freq = jnp.where(lane % 64 == k, jnp.float32(value), freq)
        for k in range(3):
            position = jnp.zeros((4, HD), jnp.int32)
            for r in range(4):
                here = len_smem[r] % STRETCH if k == 0 else pos_smem[k - 1, r]
                position = jnp.where(row == r, here, position)
            angle = position.astype(F32) * freq
            turn_ref[k, 0] = jnp.cos(angle)
            sine = jnp.sin(angle)
            turn_ref[k, 1] = jnp.where(lane < 64, -sine, sine)

    def tiles_of(kind, ty, tcore):
        t = ty * 2 + tcore
        return (24 + 2 * t, 2) if kind == 0 else (2 * t, 2) if kind == 1 else (16 + 4 * tcore + ty, 1)

    def place_of(kind, tcore):
        return (0, 2) if kind == 0 else (2, 2) if kind == 1 else (4 + tcore, 1)

    def traded(kind, dy, dc):
        ty, tcore = (y + dy) % 4, (core + dc) % 2
        first, count = tiles_of(kind, ty, tcore)
        to, _ = place_of(kind, tcore)
        src = tiles_ref.at[pl.ds(first, count)]
        dst = w_ref.at[pl.ds(to, count), seq, tp, roll]
        return remote(src, dst, trade_send.at[kind], trade_recv.at[kind, dy * 2 + dc], (x, ty, z, tcore))

    def got_trade(kind, steps):
        to, count = place_of(kind, core)
        for dy, dc in steps:
            if (dy, dc) != (0, 0):
                source = ((y - dy) % 4) * 2 + (core + dc) % 2
                here = w_ref.at[pl.ds(to, count), seq, source, roll]
                remote(here, here, trade_send.at[kind], trade_recv.at[kind, dy * 2 + dc], tp_peer(dy, dc)).wait_recv()

    def keep_own(kind):
        first, count = tiles_of(kind, y, core)
        to, _ = place_of(kind, core)
        for k in range(count):
            w_ref[to + k, seq, tp, roll] = tiles_ref[first + k]

    def trade_start(kind):
        traded(kind, 0, 1).start()
        for dy, dc in TP_STEPS:
            if dy != 0:
                traded(kind, dy, dc).start()

    loads[0].wait()
    stage(qkv_in, 0, 16)
    keep_own(1)
    pl.semaphore_wait(barrier, len(partners))
    trade_start(1)
    for dx in (1, 2, 3):
        pl.semaphore_signal(line_sem, inc=1, device_id=device(*plane_peer(dx, 0)), device_id_type=MESH)
    stage(qkv_in, 16, 8)
    keep_own(2)
    trade_start(2)
    for k in range(2, 7):
        loads[k].wait()
    select_rows()
    across = remote(normed_ref.at[1], other, other_sem.at[0], other_sem.at[1], plane_peer(2, 0))
    across.start()
    loads[1].wait()
    stage(out_in, 24, 16)
    keep_own(0)
    trade_start(0)
    tables()
    bias_ref[...] = bias_in[...].astype(F32)

    def region(kind, half):
        if kind < 2:
            return kind * 2 + half, 0, 8
        return 4 + core, half * 4, 4

    def block_at(kind, half, bx, bz, part_of):
        tile, first, count = region(kind, half)
        if part_of is not None:
            count = count // 2
            first = first + part_of * count
        return w_ref.at[pl.ds(tile, 1), (bx % 2) * 4 + bz, pl.ds(first, count), bx // 2]

    def coords(half, f, g):
        return ((x + g) % 4, (z + f) % 4) if half == 0 else ((x + f) % 4, (z + g) % 4)

    def ring(kind, half, message, f, g, part_of, step):
        bx, bz = coords(half, f, g)
        tx, tz = coords(half, *step)
        block = block_at(kind, half, bx, bz, part_of)
        return remote(block, block, ring_send.at[kind], ring_recv.at[kind, half * 20 + message], (tx, y, tz, core))

    def to_pair(kind, half, f, g, part_of=None):
        if kind == 2:
            bx, bz = coords(half, f, g)
            block = block_at(kind, half, bx, bz, part_of)
            remote(block, block, pair_sem.at[0], pair_sem.at[1], tp_peer(0, 1)).start()

    def sideways(kind, half, f):
        k = 4 + ORDER.index(f) * 4
        ring(kind, half, k, f, 0, None, (0, 1)).start()
        ring(kind, half, k + 1, f, 0, None, (0, -1)).start()

    def own_rows(kind, dys):
        for message, along in ((0, (1, 0)), (1, (-1, 0)), (4, (0, 1)), (5, (0, -1))):
            for half in (0, 1):
                tx, tz = coords(half, *along)
                tile, _, _ = region(kind, half)
                for dy in dys:
                    first = ((y - dy) % 4) * 2
                    block = w_ref.at[pl.ds(tile, 1), seq, pl.ds(first, 2), roll]
                    if kind == 2:
                        continue
                    remote(
                        block, block, ring_send.at[kind], ring_recv.at[kind, half * 20 + message], (tx, y, tz, core)
                    ).start()
                if kind == 2 and 0 not in dys:
                    block = block_at(kind, half, x, z, None)
                    remote(
                        block, block, ring_send.at[kind], ring_recv.at[kind, half * 20 + message], (tx, y, tz, core)
                    ).start()
        if kind == 2 and 0 not in dys:
            for half in (0, 1):
                to_pair(kind, half, 0, 0)

    def first_step(kind, half, f):
        ring(kind, half, 0 if f < 0 else 1, f, 0, None, (1, 0)).wait_recv()
        if f < 0:
            ring(kind, half, 2, f, 0, 0, (1, 0)).start()
        else:
            ring(kind, half, 3, f, 0, 1, (-1, 0)).start()
        sideways(kind, half, f)
        to_pair(kind, half, f, 0)

    def far_step(kind, half):
        ring(kind, half, 2, 2, 0, 0, (1, 0)).wait_recv()
        ring(kind, half, 3, 2, 0, 1, (1, 0)).wait_recv()
        sideways(kind, half, 2)
        to_pair(kind, half, 2, 0)

    def side_step(kind, half, f, g):
        k = 4 + ORDER.index(f) * 4
        if g < 0:
            ring(kind, half, k, f, -1, None, (0, 1)).wait_recv()
            ring(kind, half, k + 2, f, -1, 0, (0, 1)).start()
        else:
            ring(kind, half, k + 1, f, 1, None, (0, 1)).wait_recv()
            ring(kind, half, k + 3, f, 1, 1, (0, -1)).start()
        to_pair(kind, half, f, g)

    def last_step(kind):
        for f in ORDER:
            for half in (0, 1):
                k = 4 + ORDER.index(f) * 4
                ring(kind, half, k + 2, f, 2, 0, (0, 1)).wait_recv()
                to_pair(kind, half, f, 2, 0)
                ring(kind, half, k + 3, f, 2, 1, (0, 1)).wait_recv()
                to_pair(kind, half, f, 2, 1)

    def sent_ring(kind):
        sent = w_ref.at[0:5, 0 : (6 if kind < 2 else 3), :, 0]
        remote(sent, sent, ring_send.at[kind], ring_recv.at[kind, 0], plane_peer(0, 1)).wait_send()

    def tp_send(stage, src_of, dst, sems):
        for dy, dc in TP_STEPS:
            if (dy, dc) != (0, 0):
                target = tp_peer(dy, dc)
                remote(src_of(target[1] * 2 + target[3]), dst, stage_send.at[stage], sems.at[dy * 2 + dc], target).start()

    def tp_wait(stage, buffer, sems):
        for dy, dc in TP_STEPS:
            if (dy, dc) != (0, 0):
                here = buffer.at[((y - dy) % 4) * 2 + (core + dc) % 2]
                remote(here, here, stage_send.at[stage], sems.at[dy * 2 + dc], tp_peer(dy, dc)).wait_recv()

    def sent_all(stage, buffer, count):
        sent = buffer.at[0:count]
        remote(sent, sent, stage_send.at[stage], recv3.at[0], tp_peer(0, 1)).wait_send()

    def project():
        across.wait_recv()
        for k in range(3):
            tile = (2 + k) if k < 2 else 4 + core
            rows = w_ref[tile, seq, :, roll]
            wq[:, k * HD : (k + 1) * HD] = rows.reshape(8 * ROWS, HD)
        for k, lhs in ((0, normed_ref[0]), (1, other[...])):
            made = jnp.dot(lhs, wq[...], preferred_element_type=F32)
            part[k] = made[0:4]
        r2[x * 4 + z] = part[0]
        pl.semaphore_wait(line_sem, 3)
        for dx, dz in PLANE_STEPS:
            if (dx, dz) != (0, 0):
                tx, _, tz, _ = plane_peer(dx, dz)
                remote(
                    part.at[(tx // 2 + roll) % 2], r2.at[x * 4 + z], stage_send.at[0],
                    recv2.at[dx * 4 + dz], (tx, y, tz, core),
                ).start()

    def share():
        for dx, dz in PLANE_STEPS:
            if (dx, dz) != (0, 0):
                here = r2.at[((x - dx) % 4) * 4 + (z - dz) % 4]
                remote(here, here, stage_send.at[0], recv2.at[dx * 4 + dz], plane_peer(dx, dz)).wait_recv()
        total = r2[0]
        for k in range(1, 16):
            total = total + r2[k]
        for k in range(3):
            row = (2 * tp + k) if k < 2 else 16 + 4 * core + y
            qb[tp, k] = (total[:, k * HD : (k + 1) * HD] + bias_ref[pl.ds(row, 1)]).astype(BF16)
        tp_send(1, lambda t: qb.at[tp], qb.at[tp], recv3)

    def turn(v, position):
        return v * turn_ref[position, 0] + pltpu.roll(v, 64, v.ndim - 1) * turn_ref[position, 1]

    def queries():
        tp_wait(1, qb, recv3)
        for g in range(KVH):
            fresh_key = turn(qb[2 * g, 2].astype(F32), 0).astype(BF16)
            fresh_ref[:, g * HD : (g + 1) * HD] = fresh_key
            fresh_ref[:, (KVH + g) * HD : (KVH + g + 1) * HD] = qb[2 * g + 1, 2]
            for h in range(4 * g, 4 * g + 4):
                q = qb[h // 2, h % 2].astype(F32)
                own = turn(q, 0).astype(BF16).astype(F32)
                score = jnp.sum(own * fresh_key.astype(F32), axis=1, keepdims=True) * HD ** (-0.5)
                self_s[4 * h : 4 * h + 4] = jnp.broadcast_to(score, (4, HD))
                for b in range(2):
                    rot[b, 4 * h : 4 * h + 4] = turn(q, 1 + b)

    def scores():
        start = (seq * 8 + tp) * HERE
        owner = lax.broadcasted_iota(jnp.int32, (16, BLOCK), 0) % 4
        column = lax.broadcasted_iota(jnp.int32, (16, BLOCK), 1)
        for r in range(4):
            caches[r].wait()
            for b in range(2):
                valid = (owner == r) & (column + (start + b * BLOCK) < len_smem[r])
                for g in range(KVH):
                    rows, cols = slice(16 * g, 16 * g + 16), slice(b * BLOCK, (b + 1) * BLOCK)
                    made = lax.dot_general(
                        rot[b, rows].astype(BF16), kbuf[r, cols, g * HD : (g + 1) * HD],
                        (((1,), (1,)), ((), ())), preferred_element_type=F32,
                    )
                    before = s_buf[rows, cols] if r > 0 else jnp.full((16, BLOCK), lowest, F32)
                    s_buf[rows, cols] = jnp.where(valid, made * HD ** (-0.5), before)

    left = lax.broadcasted_iota(jnp.int32, (8, HD), 1) < HD // 2

    def values():
        for g in range(KVH):
            s = s_buf[16 * g : 16 * g + 16]
            top = jnp.maximum(jnp.max(s, axis=1, keepdims=True), floor_top)
            w = jnp.exp(s - top)
            p_buf[16 * g : 16 * g + 16] = w.astype(BF16)
            low = jnp.sum(w, axis=1, keepdims=True)
            for k in range(2):
                rows = slice(8 * k, 8 * k + 8)
                ob[2 * g + k, 0] = jnp.where(left, top[rows], low[rows])
        owner = lax.broadcasted_iota(jnp.int32, (16, HERE), 0) % 4
        for r in range(4):
            caches[4 + r].wait()
        for g in range(KVH):
            total = jnp.zeros((16, HD), F32)
            w = p_buf[16 * g : 16 * g + 16].astype(F32)
            for r in range(4):
                mine = jnp.where(owner == r, w, 0.0).astype(BF16)
                total += jnp.dot(mine, vbuf[r, :, g * HD : (g + 1) * HD], preferred_element_type=F32)
            ob[2 * g, 1] = total[0:8]
            ob[2 * g + 1, 1] = total[8:16]
        r5[tp] = ob[tp]
        tp_send(2, lambda t: ob.at[t], r5.at[tp], recv5)

    def combined(buffer):
        tiles = [(buffer[k, 0], pltpu.roll(buffer[k, 0], 64, 1)) for k in range(8)]
        tops = [jnp.where(left, one, two) for one, two in tiles]
        top = tops[0]
        for k in range(1, 8):
            top = jnp.maximum(top, tops[k])
        low, out = jnp.zeros_like(top), jnp.zeros_like(top)
        for k in range(8):
            factor = jnp.exp(tops[k] - top)
            low += jnp.where(left, tiles[k][1], tiles[k][0]) * factor
            out += buffer[k, 1] * factor
        return top, low, out

    def over_tp():
        tp_wait(2, r5, recv5)
        top, low, out = combined(r5)
        for k, value in enumerate((jnp.where(left, top, low), out)):
            c6[k] = value
            r6[seq, k] = value
        for dl in range(2):
            for dz in (2, 1, 3, 0):
                if dl + dz > 0:
                    tx, tz = roll * 2 + (x + dl) % 2, (z + dz) % 4
                    remote(c6, r6.at[seq], stage_send.at[3], recv6.at[dl * 4 + dz], (tx, y, tz, core)).start()

    def finish():
        for dl in range(2):
            for dz in (2, 1, 3, 0):
                if dl + dz > 0:
                    here = r6.at[((x + dl) % 2) * 4 + (z - dz) % 4]
                    remote(here, here, stage_send.at[3], recv6.at[dl * 4 + dz], plane_peer(0, 1)).wait_recv()
        old_top, old_low, old_out = combined(r6)
        mine = self_s[pl.ds(pl.multiple_of(tp * 8, 8), 8)]
        top = jnp.maximum(old_top, mine)
        factor, fresh = jnp.exp(old_top - top), jnp.exp(mine - top)
        own_value = qb[(tp // 2) * 2 + 1, 2].astype(F32)
        both = jnp.concatenate([own_value, own_value], axis=0)
        numerator = old_out * factor + fresh.astype(BF16).astype(F32) * both
        attention = (numerator / (old_low * factor + fresh)).astype(BF16)
        return attention

    def stage_out():
        for o in range(8):
            for k in range(2):
                wo[k, o] = w_ref[k, o].reshape(16 * ROWS, HD)

    def out_project(attention):
        for o in range(8):
            sums = []
            for k in range(2):
                sums.append(lax.dot_general(attention, wo[k, o], (((1,), (1,)), ((), ())), preferred_element_type=F32))
            po[o, :, 0:448] = sums[0][0:4] + sums[1][4:8]
            po[o, :, 448:512] = jnp.zeros((4, 64), F32)
        r7[tp] = po[tp]
        tp_send(4, lambda t: po.at[t], r7.at[tp], recv7)

    def reduce_out():
        tp_wait(4, r7, recv7)
        total = r7[0]
        for k in range(1, 8):
            total = total + r7[k]
        final_ref[tp] = total.astype(BF16)
        tp_send(5, lambda t: final_ref.at[tp], final_ref.at[tp], recv8)

    pair, rest = ((0, 1),), tuple((dy, dc) for dy, dc in TP_STEPS if dy)
    had = set()

    def need(kind, *parts):
        for name, steps in (("pair", pair), ("rest", rest)):
            if name in parts and (kind, name) not in had:
                had.add((kind, name))
                got_trade(kind, steps)

    for name, *at in STEPS:
        if name == "ownA":
            need(at[0], "pair")
            own_rows(at[0], (0,))
        elif name == "ownB":
            need(at[0], "pair", "rest")
            own_rows(at[0], (3, 1, 2))
        elif name == "f1p":
            first_step(*at, -1)
        elif name == "f1m":
            first_step(*at, 1)
        elif name == "f2":
            far_step(*at)
        elif name == "gp":
            side_step(*at, -1)
        elif name == "gm":
            side_step(*at, 1)
        elif name == "project":
            need(1, "pair", "rest")
            need(2, "pair", "rest")
            project()
        elif name == "share":
            share()
        elif name == "queries":
            queries()
        elif name == "scores":
            scores()
        elif name == "values":
            values()
        elif name == "over_tp":
            over_tp()
        elif name == "stage_out":
            last_step(0)
            stage_out()
        elif name == "out_project":
            out_project(finish())
        elif name == "reduce_out":
            reduce_out()
    last_step(1)
    last_step(2)
    for kind in range(3):
        sent_ring(kind)
    tile = w_ref.at[5 - core]
    whole = remote(tile, tile, pair_sem.at[0], pair_sem.at[1], tp_peer(0, 1))
    whole.wait_send()
    whole.wait_recv()
    tp_wait(5, final_ref, recv8)
    for kind in range(3):
        sent = tiles_ref.at[0 : (14 if kind < 2 else 7)]
        remote(sent, sent, trade_send.at[kind], trade_recv.at[kind, 1], tp_peer(0, 1)).wait_send()
    across.wait_send()
    sent_all(0, r2, 15)
    sent_all(1, qb, 7)
    sent_all(2, ob, 7)
    sent_all(3, r6, 7)
    sent_all(4, po, 7)
    sent_all(5, final_ref, 7)


def layer(hidden, gain, bias, qkv_rows, out_rows, lengths, positions, keys, values):
    hbm, vmem = pl.BlockSpec(memory_space=pltpu.HBM), pl.BlockSpec(memory_space=pltpu.VMEM)
    dma = pltpu.SemaphoreType.DMA
    return pl.pallas_call(
        layer_kernel,
        name="layer",
        out_shape=(
            jax.ShapeDtypeStruct((6, 8, 8, 2, GROUPS, 4, HD), BF16),
            jax.ShapeDtypeStruct((4, 2 * KVH * HD), BF16),
            jax.ShapeDtypeStruct((8, 4, 512), BF16),
        ),
        in_specs=[hbm] * 9,
        out_specs=(vmem, vmem, vmem),
        scratch_shapes=[
            pltpu.SMEM((4,), jnp.int32),
            pltpu.SMEM((2, 4), jnp.int32),
            pltpu.VMEM((4, 3584), BF16),
            pltpu.VMEM((3584,), BF16),
            pltpu.VMEM((1, 3584), F32),
            pltpu.VMEM((24, HD), BF16),
            pltpu.VMEM((ROWS, 24 * HD), BF16),
            pltpu.VMEM((ROWS, 16 * HD), BF16),
            pltpu.VMEM((40, GROUPS, 4, HD), BF16),
            pltpu.VMEM((8, 512), F32),
            pltpu.VMEM((24, HD), F32),
            pltpu.VMEM((3, 2, 4, HD), F32),
            pltpu.VMEM((4, HERE, KVH * HD), BF16),
            pltpu.VMEM((4, HERE, KVH * HD), BF16),
            pltpu.VMEM((2, 8, 8 * ROWS), BF16),
            pltpu.VMEM((8, 8 * ROWS), BF16),
            pltpu.VMEM((2, 8, 16 * ROWS, HD), BF16),
            pltpu.VMEM((8 * ROWS, 3 * HD), BF16),
            pltpu.VMEM((2, 4, 3 * HD), F32),
            pltpu.VMEM((16, 4, 3 * HD), F32),
            pltpu.VMEM((8, 3, 4, HD), BF16),
            pltpu.VMEM((2, 64, HD), F32),
            pltpu.VMEM((64, HD), F32),
            pltpu.VMEM((64, HERE), F32),
            pltpu.VMEM((64, HERE), BF16),
            pltpu.VMEM((8, 2, 8, HD), F32),
            pltpu.VMEM((8, 2, 8, HD), F32),
            pltpu.VMEM((2, 8, HD), F32),
            pltpu.VMEM((8, 2, 8, HD), F32),
            pltpu.VMEM((8, 4, 512), F32),
            pltpu.VMEM((8, 4, 512), F32),
            pltpu.SemaphoreType.REGULAR, dma((7,)), dma((2, 4)), dma((3,)), dma((3, 8)), dma((3,)), dma((3, 40)), dma((2,)), dma((2,)),
            dma((6,)), dma((16,)), dma((8,)), dma((8,)), dma((8,)), dma((8,)), dma((8,)),
        ],
        compiler_params=pltpu.CompilerParams(
            collective_id=0, has_side_effects=True, vmem_limit_bytes=40 * 2**20
        ),
    )(hidden, gain, bias, qkv_rows, out_rows, lengths, positions, keys, values)


def place_kernel(w_ref, fresh_ref, final_ref, attended_out, fresh_out, qkv_ref, out_ref, attended_ref, sems, small):
    copies = []
    for k in range(6):
        target = out_ref.at[:, k * HD : (k + 1) * HD] if k < 2 else qkv_ref.at[:, (k - 2) * HD : (k - 1) * HD]
        for part in range(PLACE):
            rows = slice(part * 3584 // PLACE, (part + 1) * 3584 // PLACE)
            copies.append(pltpu.make_async_copy(w_ref.at[k, rows], target.at[rows], sems.at[k, part]))
    for copy in copies:
        copy.start()
    copies.append(pltpu.make_async_copy(fresh_ref, fresh_out, small.at[0]))
    copies[-1].start()
    for o in range(8):
        attended_ref[:, o * 448 : (o + 1) * 448] = final_ref[o, :, 0:448]
    copies.append(pltpu.make_async_copy(attended_ref, attended_out, small.at[1]))
    copies[-1].start()
    for copy in copies:
        copy.wait()


def place(w, fresh, final):
    hbm, vmem = pl.BlockSpec(memory_space=pltpu.HBM), pl.BlockSpec(memory_space=pltpu.VMEM)
    return pl.pallas_call(
        place_kernel,
        name="place",
        out_shape=(
            jax.ShapeDtypeStruct((4, 3584), BF16),
            jax.ShapeDtypeStruct((4, 1024), BF16),
            jax.ShapeDtypeStruct((3584, 512), BF16),
            jax.ShapeDtypeStruct((3584, 256), BF16),
        ),
        in_specs=[vmem, vmem, vmem],
        out_specs=(hbm, hbm, hbm, hbm),
        scratch_shapes=[
            pltpu.VMEM((4, 3584), BF16), pltpu.SemaphoreType.DMA((6, PLACE)), pltpu.SemaphoreType.DMA((2,)),
        ],
        compiler_params=pltpu.CompilerParams(vmem_limit_bytes=8 * 2**20),
    )(w, fresh, final)


def body(
    hidden,
    norm_gain,
    qkv_bias,
    qkv_weight,
    out_weight,
    key_cache,
    value_cache,
    cache_len,
    block_pos,
):
    operands = (
        hidden, norm_gain, qkv_bias.reshape(24, HD), qkv_weight, out_weight,
        cache_len, block_pos.T, key_cache, value_cache,
    )
    w, fresh_kv, final = layer(*(pltpu.with_memory_space_constraint(a, pltpu.HBM) for a in operands))
    return place(w.reshape(6, 3584, HD), fresh_kv, final)


def solution(mesh):
    finer = Mesh(
        mesh.devices.reshape(2, 4, 4, 2, mesh.shape["roll"]),
        ("seq_0", "seq_1", "tp_0", "tp_1", "roll"),
    )
    in_specs = (
        P("roll", None),
        P(),
        P(),
        P(SEQ_TP_ROLL, None),
        P(SEQ_TP_ROLL, None),
        P("roll", SEQ_TP, None),
        P("roll", SEQ_TP, None),
        P("roll"),
        P("roll", SEQ_TP),
    )
    out_specs = (P("roll", None), P("roll", None), P(None, TP), P(None, TP))
    return jax.shard_map(body, mesh=finer, in_specs=in_specs, out_specs=out_specs, check_vma=False)
```

```python
import jax
import jax.numpy as jnp
import numpy as np
from jax import lax
from jax.experimental import pallas as pl
from jax.experimental.pallas import tpu as pltpu
from jax.sharding import Mesh
from jax.sharding import PartitionSpec as P

HQ = 16
KVH = 4
HD = 128
BLOCK = 512
STRETCH = 8192
ROWS = 28
PLACE = 4
GROUPS = 7
HERE = 1024
TP = ("tp_0", "tp_1")
SEQ = ("seq_0", "seq_1")
SEQ_TP = ("seq_0", "seq_1", "tp_0", "tp_1")
SEQ_TP_ROLL = ("seq_0", "seq_1", "tp_0", "tp_1", "roll")
MESH = pl.DeviceIdType.MESH
F32 = jnp.float32
BF16 = jnp.bfloat16

rope_base = 10000000.0
norm_eps = 1e-06
lowest = -1e30
floor_top = -1e20


def frequencies(width):
    half_width = width // 2
    exact = rope_base ** (-2.0 * np.arange(half_width) / width)
    octave = np.floor(np.log2(exact))
    quantum = 2.0 ** (8.0 - octave)
    return np.floor(exact * quantum) / quantum


def device(x, y, z, core):
    return (x % 2, z, y, core, x // 2)


ORDER = (0, -1, 1, 2)
TP_STEPS = tuple((dy, dc) for dy in (0, 2, 3, 1) for dc in (0, 1))
PLANE_STEPS = tuple((dx, dz) for dx in (2, 1, 3, 0) for dz in (2, 1, 3, 0))


STEPS = (
    ("ownA", 1), ("ownA", 0), ("ownB", 1), ("ownB", 2), ("ownB", 0), ("project",), ("gp", 2, 0, 0),
    ("f1m", 0, 1), ("f1p", 0, 0), ("f1p", 0, 1), ("gm", 1, 0, 0), ("gp", 0, 1, 0), ("gp", 2, 1, 0),
    ("f1m", 0, 0), ("f1m", 2, 0), ("f1p", 1, 1), ("share",), ("f1m", 1, 1), ("f1p", 2, 0), ("f2", 0, 1),
    ("f1m", 1, 0), ("f1p", 2, 1), ("gp", 0, 1, -1), ("f1m", 2, 1), ("gm", 0, 1, 0), ("f2", 0, 0),
    ("gm", 0, 0, 1), ("f1p", 1, 0), ("gm", 0, 1, -1), ("gp", 0, 1, 1), ("gp", 0, 0, -1), ("gm", 2, 0, 0),
    ("queries",), ("scores",), ("values",), ("gm", 0, 0, 0), ("gm", 0, 0, -1), ("f2", 1, 1), ("gp", 2, 0, -1),
    ("f2", 2, 0), ("gp", 0, 0, 2), ("gm", 0, 1, 2), ("gp", 0, 0, 0), ("gp", 0, 1, 2), ("f2", 2, 1),
    ("gm", 0, 0, 2), ("gp", 0, 0, 1), ("gm", 0, 1, 1), ("over_tp",), ("f2", 1, 0), ("gp", 2, 1, 1),
    ("gm", 2, 0, -1), ("gm", 1, 1, 1), ("gm", 1, 1, 2), ("gp", 2, 1, -1), ("gp", 2, 0, 2), ("gp", 1, 0, 0),
    ("gp", 1, 1, 1), ("gm", 1, 1, -1), ("gm", 2, 1, 0), ("gp", 1, 0, 1), ("gm", 2, 1, 1), ("gm", 2, 0, 2),
    ("gp", 1, 1, 0), ("gm", 1, 0, -1), ("gm", 2, 1, -1), ("gp", 1, 0, -1), ("gp", 1, 1, -1), ("stage_out",),
    ("out_project",), ("gm", 2, 0, 1), ("gp", 2, 0, 1), ("gm", 1, 1, 0), ("gp", 2, 1, 2), ("gm", 1, 0, 1),
    ("gp", 1, 1, 2), ("gm", 2, 1, 2), ("gp", 1, 0, 2), ("gm", 1, 0, 2), ("reduce_out",),
)


def layer_kernel(
    hidden_ref, gain_ref, bias_hbm, qkv_ref, out_ref, len_ref, pos_ref, key_ref, value_ref,
    w_ref, fresh_ref, final_ref,
    len_smem, pos_smem, hidden_in, gain_in, gain_row, bias_in, qkv_in, out_in, tiles_ref, near, bias_ref, turn_ref,
    kbuf, vbuf, normed_ref, other, wo, wq, part, r2, qb, rot, self_s, s_buf, p_buf, ob, r5, c6, r6, po, r7,
    line_sem, load_sem, cache_sem, trade_send, trade_recv, ring_send, ring_recv, pair_sem, other_sem,
    stage_send, recv2, recv3, recv5, recv6, recv7, recv8,
):
    x = lax.axis_index("roll") * 2 + lax.axis_index("seq_0")
    y, z, core = lax.axis_index("tp_0"), lax.axis_index("seq_1"), lax.axis_index("tp_1")
    seq, roll, tp = (x % 2) * 4 + z, x // 2, y * 2 + core

    def remote(src, dst, send, recv, target):
        return pltpu.make_async_remote_copy(
            src_ref=src, dst_ref=dst, send_sem=send, recv_sem=recv,
            device_id=device(*target), device_id_type=MESH,
        )

    def tp_peer(dy, dc):
        return (x, (y + dy) % 4, z, (core + dc) % 2)

    def plane_peer(dx, dz):
        return ((x + dx) % 4, y, (z + dz) % 4, core)

    partners = [tp_peer(dy, dc) for dy, dc in TP_STEPS if (dy, dc) != (0, 0)]
    partners += [plane_peer(dx, dz) for dx, dz in PLANE_STEPS if (dx == 0) != (dz == 0)]

    caches = []
    for r in range(4):
        caches.append(pltpu.make_async_copy(key_ref.at[r], kbuf.at[r], cache_sem.at[0, r]))
    for r in range(4):
        caches.append(pltpu.make_async_copy(value_ref.at[r], vbuf.at[r], cache_sem.at[1, r]))

    barrier = pltpu.get_barrier_semaphore()
    for partner in partners:
        pl.semaphore_signal(barrier, inc=1, device_id=device(*partner), device_id_type=MESH)
    loads = [
        pltpu.make_async_copy(src, dst, load_sem.at[k])
        for k, (src, dst) in enumerate((
            (qkv_ref, qkv_in), (out_ref, out_in), (hidden_ref, hidden_in), (gain_ref, gain_in), (bias_hbm, bias_in),
            (len_ref, len_smem), (pos_ref, pos_smem),
        ))
    ]
    for copy in loads + caches:
        copy.start()

    def stage(source, first, count):
        start = first % 24
        for k in range(start, start + count):
            tiles_ref[first + k - start] = source[:, k * HD : (k + 1) * HD].reshape(GROUPS, 4, HD)

    def select_rows():
        wide = hidden_in[...].astype(F32)
        scale = lax.rsqrt(jnp.sum(wide * wide, axis=1, keepdims=True) * (1.0 / 3584) + norm_eps)
        gain_row[...] = gain_in[...].astype(F32).reshape(1, 3584)
        base = pl.multiple_of(((7 * seq) // 2) * HD, HD)
        wide = hidden_in[:, pl.ds(base, 512)].astype(F32) * scale * gain_row[:, pl.ds(base, 512)]
        near[0:4] = wide
        near[4:8] = jnp.zeros((4, 512), F32)
        lhs = near[...].astype(BF16)
        feature = lax.broadcasted_iota(jnp.int32, (512, 8 * ROWS), 0) + (base - seq * 448)
        column = lax.broadcasted_iota(jnp.int32, (512, 8 * ROWS), 1)
        wanted = column + (column // ROWS) * ROWS
        for k, r in ((0, roll), (1, 1 - roll)):
            picked = jnp.where(feature == wanted + r * ROWS, 1.0, 0.0).astype(BF16)
            normed_ref[k] = jnp.dot(lhs, picked, preferred_element_type=F32).astype(BF16)

    def tables():
        lane = lax.broadcasted_iota(jnp.int32, (4, HD), 1)
        row = lax.broadcasted_iota(jnp.int32, (4, HD), 0)
        freq = jnp.zeros((4, HD), F32)
        for k, value in enumerate(frequencies(HD)):
            freq = jnp.where(lane % 64 == k, jnp.float32(value), freq)
        for k in range(3):
            position = jnp.zeros((4, HD), jnp.int32)
            for r in range(4):
                here = len_smem[r] % STRETCH if k == 0 else pos_smem[k - 1, r]
                position = jnp.where(row == r, here, position)
            angle = position.astype(F32) * freq
            turn_ref[k, 0] = jnp.cos(angle)
            sine = jnp.sin(angle)
            turn_ref[k, 1] = jnp.where(lane < 64, -sine, sine)

    def tiles_of(kind, ty, tcore):
        t = ty * 2 + tcore
        return (24 + 2 * t, 2) if kind == 0 else (2 * t, 2) if kind == 1 else (16 + 4 * tcore + ty, 1)

    def place_of(kind, tcore):
        return (0, 2) if kind == 0 else (2, 2) if kind == 1 else (4 + tcore, 1)

    def traded(kind, dy, dc):
        ty, tcore = (y + dy) % 4, (core + dc) % 2
        first, count = tiles_of(kind, ty, tcore)
        to, _ = place_of(kind, tcore)
        src = tiles_ref.at[pl.ds(first, count)]
        dst = w_ref.at[pl.ds(to, count), seq, tp, roll]
        return remote(src, dst, trade_send.at[kind], trade_recv.at[kind, dy * 2 + dc], (x, ty, z, tcore))

    def got_trade(kind, steps):
        to, count = place_of(kind, core)
        for dy, dc in steps:
            if (dy, dc) != (0, 0):
                source = ((y - dy) % 4) * 2 + (core + dc) % 2
                here = w_ref.at[pl.ds(to, count), seq, source, roll]
                remote(here, here, trade_send.at[kind], trade_recv.at[kind, dy * 2 + dc], tp_peer(dy, dc)).wait_recv()

    def keep_own(kind):
        first, count = tiles_of(kind, y, core)
        to, _ = place_of(kind, core)
        for k in range(count):
            w_ref[to + k, seq, tp, roll] = tiles_ref[first + k]

    def trade_start(kind):
        traded(kind, 0, 1).start()
        for dy, dc in TP_STEPS:
            if dy != 0:
                traded(kind, dy, dc).start()

    loads[0].wait()
    stage(qkv_in, 0, 16)
    keep_own(1)
    pl.semaphore_wait(barrier, len(partners))
    trade_start(1)
    for dx in (1, 2, 3):
        pl.semaphore_signal(line_sem, inc=1, device_id=device(*plane_peer(dx, 0)), device_id_type=MESH)
    stage(qkv_in, 16, 8)
    keep_own(2)
    trade_start(2)
    for k in range(2, 7):
        loads[k].wait()
    select_rows()
    across = remote(normed_ref.at[1], other, other_sem.at[0], other_sem.at[1], plane_peer(2, 0))
    across.start()
    loads[1].wait()
    stage(out_in, 24, 16)
    keep_own(0)
    trade_start(0)
    tables()
    bias_ref[...] = bias_in[...].astype(F32)

    def region(kind, half):
        if kind < 2:
            return kind * 2 + half, 0, 8
        return 4 + core, half * 4, 4

    def block_at(kind, half, bx, bz, part_of):
        tile, first, count = region(kind, half)
        if part_of is not None:
            count = count // 2
            first = first + part_of * count
        return w_ref.at[pl.ds(tile, 1), (bx % 2) * 4 + bz, pl.ds(first, count), bx // 2]

    def coords(half, f, g):
        return ((x + g) % 4, (z + f) % 4) if half == 0 else ((x + f) % 4, (z + g) % 4)

    def ring(kind, half, message, f, g, part_of, step):
        bx, bz = coords(half, f, g)
        tx, tz = coords(half, *step)
        block = block_at(kind, half, bx, bz, part_of)
        return remote(block, block, ring_send.at[kind], ring_recv.at[kind, half * 20 + message], (tx, y, tz, core))

    def to_pair(kind, half, f, g, part_of=None):
        if kind == 2:
            bx, bz = coords(half, f, g)
            block = block_at(kind, half, bx, bz, part_of)
            remote(block, block, pair_sem.at[0], pair_sem.at[1], tp_peer(0, 1)).start()

    def sideways(kind, half, f):
        k = 4 + ORDER.index(f) * 4
        ring(kind, half, k, f, 0, None, (0, 1)).start()
        ring(kind, half, k + 1, f, 0, None, (0, -1)).start()

    def own_rows(kind, dys):
        for message, along in ((0, (1, 0)), (1, (-1, 0)), (4, (0, 1)), (5, (0, -1))):
            for half in (0, 1):
                tx, tz = coords(half, *along)
                tile, _, _ = region(kind, half)
                for dy in dys:
                    first = ((y - dy) % 4) * 2
                    block = w_ref.at[pl.ds(tile, 1), seq, pl.ds(first, 2), roll]
                    if kind == 2:
                        continue
                    remote(
                        block, block, ring_send.at[kind], ring_recv.at[kind, half * 20 + message], (tx, y, tz, core)
                    ).start()
                if kind == 2 and 0 not in dys:
                    block = block_at(kind, half, x, z, None)
                    remote(
                        block, block, ring_send.at[kind], ring_recv.at[kind, half * 20 + message], (tx, y, tz, core)
                    ).start()
        if kind == 2 and 0 not in dys:
            for half in (0, 1):
                to_pair(kind, half, 0, 0)

    def first_step(kind, half, f):
        ring(kind, half, 0 if f < 0 else 1, f, 0, None, (1, 0)).wait_recv()
        if f < 0:
            ring(kind, half, 2, f, 0, 0, (1, 0)).start()
        else:
            ring(kind, half, 3, f, 0, 1, (-1, 0)).start()
        sideways(kind, half, f)
        to_pair(kind, half, f, 0)

    def far_step(kind, half):
        ring(kind, half, 2, 2, 0, 0, (1, 0)).wait_recv()
        ring(kind, half, 3, 2, 0, 1, (1, 0)).wait_recv()
        sideways(kind, half, 2)
        to_pair(kind, half, 2, 0)

    def side_step(kind, half, f, g):
        k = 4 + ORDER.index(f) * 4
        if g < 0:
            ring(kind, half, k, f, -1, None, (0, 1)).wait_recv()
            ring(kind, half, k + 2, f, -1, 0, (0, 1)).start()
        else:
            ring(kind, half, k + 1, f, 1, None, (0, 1)).wait_recv()
            ring(kind, half, k + 3, f, 1, 1, (0, -1)).start()
        to_pair(kind, half, f, g)

    def last_step(kind):
        for f in ORDER:
            for half in (0, 1):
                k = 4 + ORDER.index(f) * 4
                ring(kind, half, k + 2, f, 2, 0, (0, 1)).wait_recv()
                to_pair(kind, half, f, 2, 0)
                ring(kind, half, k + 3, f, 2, 1, (0, 1)).wait_recv()
                to_pair(kind, half, f, 2, 1)

    def sent_ring(kind):
        sent = w_ref.at[0:5, 0 : (6 if kind < 2 else 3), :, 0]
        remote(sent, sent, ring_send.at[kind], ring_recv.at[kind, 0], plane_peer(0, 1)).wait_send()

    def tp_send(stage, src_of, dst, sems):
        for dy, dc in TP_STEPS:
            if (dy, dc) != (0, 0):
                target = tp_peer(dy, dc)
                remote(src_of(target[1] * 2 + target[3]), dst, stage_send.at[stage], sems.at[dy * 2 + dc], target).start()

    def tp_wait(stage, buffer, sems):
        for dy, dc in TP_STEPS:
            if (dy, dc) != (0, 0):
                here = buffer.at[((y - dy) % 4) * 2 + (core + dc) % 2]
                remote(here, here, stage_send.at[stage], sems.at[dy * 2 + dc], tp_peer(dy, dc)).wait_recv()

    def sent_all(stage, buffer, count):
        sent = buffer.at[0:count]
        remote(sent, sent, stage_send.at[stage], recv3.at[0], tp_peer(0, 1)).wait_send()

    def project():
        across.wait_recv()
        for k in range(3):
            tile = (2 + k) if k < 2 else 4 + core
            rows = w_ref[tile, seq, :, roll]
            wq[:, k * HD : (k + 1) * HD] = rows.reshape(8 * ROWS, HD)
        for k, lhs in ((0, normed_ref[0]), (1, other[...])):
            made = jnp.dot(lhs, wq[...], preferred_element_type=F32)
            part[k] = made[0:4]
        r2[x * 4 + z] = part[0]
        pl.semaphore_wait(line_sem, 3)
        for dx, dz in PLANE_STEPS:
            if (dx, dz) != (0, 0):
                tx, _, tz, _ = plane_peer(dx, dz)
                remote(
                    part.at[(tx // 2 + roll) % 2], r2.at[x * 4 + z], stage_send.at[0],
                    recv2.at[dx * 4 + dz], (tx, y, tz, core),
                ).start()

    def share():
        for dx, dz in PLANE_STEPS:
            if (dx, dz) != (0, 0):
                here = r2.at[((x - dx) % 4) * 4 + (z - dz) % 4]
                remote(here, here, stage_send.at[0], recv2.at[dx * 4 + dz], plane_peer(dx, dz)).wait_recv()
        total = r2[0]
        for k in range(1, 16):
            total = total + r2[k]
        for k in range(3):
            row = (2 * tp + k) if k < 2 else 16 + 4 * core + y
            qb[tp, k] = (total[:, k * HD : (k + 1) * HD] + bias_ref[pl.ds(row, 1)]).astype(BF16)
        tp_send(1, lambda t: qb.at[tp], qb.at[tp], recv3)

    def turn(v, position):
        return v * turn_ref[position, 0] + pltpu.roll(v, 64, v.ndim - 1) * turn_ref[position, 1]

    def queries():
        tp_wait(1, qb, recv3)
        for g in range(KVH):
            fresh_key = turn(qb[2 * g, 2].astype(F32), 0).astype(BF16)
            fresh_ref[:, g * HD : (g + 1) * HD] = fresh_key
            fresh_ref[:, (KVH + g) * HD : (KVH + g + 1) * HD] = qb[2 * g + 1, 2]
            for h in range(4 * g, 4 * g + 4):
                q = qb[h // 2, h % 2].astype(F32)
                own = turn(q, 0).astype(BF16).astype(F32)
                score = jnp.sum(own * fresh_key.astype(F32), axis=1, keepdims=True) * HD ** (-0.5)
                self_s[4 * h : 4 * h + 4] = jnp.broadcast_to(score, (4, HD))
                for b in range(2):
                    rot[b, 4 * h : 4 * h + 4] = turn(q, 1 + b)

    def scores():
        start = (seq * 8 + tp) * HERE
        owner = lax.broadcasted_iota(jnp.int32, (16, BLOCK), 0) % 4
        column = lax.broadcasted_iota(jnp.int32, (16, BLOCK), 1)
        for r in range(4):
            caches[r].wait()
            for b in range(2):
                valid = (owner == r) & (column + (start + b * BLOCK) < len_smem[r])
                for g in range(KVH):
                    rows, cols = slice(16 * g, 16 * g + 16), slice(b * BLOCK, (b + 1) * BLOCK)
                    made = lax.dot_general(
                        rot[b, rows].astype(BF16), kbuf[r, cols, g * HD : (g + 1) * HD],
                        (((1,), (1,)), ((), ())), preferred_element_type=F32,
                    )
                    before = s_buf[rows, cols] if r > 0 else jnp.full((16, BLOCK), lowest, F32)
                    s_buf[rows, cols] = jnp.where(valid, made * HD ** (-0.5), before)

    left = lax.broadcasted_iota(jnp.int32, (8, HD), 1) < HD // 2

    def values():
        for g in range(KVH):
            s = s_buf[16 * g : 16 * g + 16]
            top = jnp.maximum(jnp.max(s, axis=1, keepdims=True), floor_top)
            w = jnp.exp(s - top)
            p_buf[16 * g : 16 * g + 16] = w.astype(BF16)
            low = jnp.sum(w, axis=1, keepdims=True)
            for k in range(2):
                rows = slice(8 * k, 8 * k + 8)
                ob[2 * g + k, 0] = jnp.where(left, top[rows], low[rows])
        owner = lax.broadcasted_iota(jnp.int32, (16, HERE), 0) % 4
        for r in range(4):
            caches[4 + r].wait()
        for g in range(KVH):
            total = jnp.zeros((16, HD), F32)
            w = p_buf[16 * g : 16 * g + 16].astype(F32)
            for r in range(4):
                mine = jnp.where(owner == r, w, 0.0).astype(BF16)
                total += jnp.dot(mine, vbuf[r, :, g * HD : (g + 1) * HD], preferred_element_type=F32)
            ob[2 * g, 1] = total[0:8]
            ob[2 * g + 1, 1] = total[8:16]
        r5[tp] = ob[tp]
        tp_send(2, lambda t: ob.at[t], r5.at[tp], recv5)

    def combined(buffer):
        tiles = [(buffer[k, 0], pltpu.roll(buffer[k, 0], 64, 1)) for k in range(8)]
        tops = [jnp.where(left, one, two) for one, two in tiles]
        top = tops[0]
        for k in range(1, 8):
            top = jnp.maximum(top, tops[k])
        low, out = jnp.zeros_like(top), jnp.zeros_like(top)
        for k in range(8):
            factor = jnp.exp(tops[k] - top)
            low += jnp.where(left, tiles[k][1], tiles[k][0]) * factor
            out += buffer[k, 1] * factor
        return top, low, out

    def over_tp():
        tp_wait(2, r5, recv5)
        top, low, out = combined(r5)
        for k, value in enumerate((jnp.where(left, top, low), out)):
            c6[k] = value
            r6[seq, k] = value
        for dl in range(2):
            for dz in (2, 1, 3, 0):
                if dl + dz > 0:
                    tx, tz = roll * 2 + (x + dl) % 2, (z + dz) % 4
                    remote(c6, r6.at[seq], stage_send.at[3], recv6.at[dl * 4 + dz], (tx, y, tz, core)).start()

    def finish():
        for dl in range(2):
            for dz in (2, 1, 3, 0):
                if dl + dz > 0:
                    here = r6.at[((x + dl) % 2) * 4 + (z - dz) % 4]
                    remote(here, here, stage_send.at[3], recv6.at[dl * 4 + dz], plane_peer(0, 1)).wait_recv()
        old_top, old_low, old_out = combined(r6)
        mine = self_s[pl.ds(pl.multiple_of(tp * 8, 8), 8)]
        top = jnp.maximum(old_top, mine)
        factor, fresh = jnp.exp(old_top - top), jnp.exp(mine - top)
        own_value = qb[(tp // 2) * 2 + 1, 2].astype(F32)
        both = jnp.concatenate([own_value, own_value], axis=0)
        numerator = old_out * factor + fresh.astype(BF16).astype(F32) * both
        attention = (numerator / (old_low * factor + fresh)).astype(BF16)
        return attention

    def stage_out():
        for o in range(8):
            for k in range(2):
                wo[k, o] = w_ref[k, o].reshape(16 * ROWS, HD)

    def out_project(attention):
        for o in range(8):
            sums = []
            for k in range(2):
                sums.append(lax.dot_general(attention, wo[k, o], (((1,), (1,)), ((), ())), preferred_element_type=F32))
            po[o, :, 0:448] = sums[0][0:4] + sums[1][4:8]
            po[o, :, 448:512] = jnp.zeros((4, 64), F32)
        r7[tp] = po[tp]
        tp_send(4, lambda t: po.at[t], r7.at[tp], recv7)

    def reduce_out():
        tp_wait(4, r7, recv7)
        total = r7[0]
        for k in range(1, 8):
            total = total + r7[k]
        final_ref[tp] = total.astype(BF16)
        tp_send(5, lambda t: final_ref.at[tp], final_ref.at[tp], recv8)

    pair, rest = ((0, 1),), tuple((dy, dc) for dy, dc in TP_STEPS if dy)
    had = set()

    def need(kind, *parts):
        for name, steps in (("pair", pair), ("rest", rest)):
            if name in parts and (kind, name) not in had:
                had.add((kind, name))
                got_trade(kind, steps)

    for name, *at in STEPS:
        if name == "ownA":
            need(at[0], "pair")
            own_rows(at[0], (0,))
        elif name == "ownB":
            need(at[0], "pair", "rest")
            own_rows(at[0], (3, 1, 2))
        elif name == "f1p":
            first_step(*at, -1)
        elif name == "f1m":
            first_step(*at, 1)
        elif name == "f2":
            far_step(*at)
        elif name == "gp":
            side_step(*at, -1)
        elif name == "gm":
            side_step(*at, 1)
        elif name == "project":
            need(1, "pair", "rest")
            need(2, "pair", "rest")
            project()
        elif name == "share":
            share()
        elif name == "queries":
            queries()
        elif name == "scores":
            scores()
        elif name == "values":
            values()
        elif name == "over_tp":
            over_tp()
        elif name == "stage_out":
            last_step(0)
            stage_out()
        elif name == "out_project":
            out_project(finish())
        elif name == "reduce_out":
            reduce_out()
    last_step(1)
    last_step(2)
    for kind in range(3):
        sent_ring(kind)
    tile = w_ref.at[5 - core]
    whole = remote(tile, tile, pair_sem.at[0], pair_sem.at[1], tp_peer(0, 1))
    whole.wait_send()
    whole.wait_recv()
    tp_wait(5, final_ref, recv8)
    for kind in range(3):
        sent = tiles_ref.at[0 : (14 if kind < 2 else 7)]
        remote(sent, sent, trade_send.at[kind], trade_recv.at[kind, 1], tp_peer(0, 1)).wait_send()
    across.wait_send()
    sent_all(0, r2, 15)
    sent_all(1, qb, 7)
    sent_all(2, ob, 7)
    sent_all(3, r6, 7)
    sent_all(4, po, 7)
    sent_all(5, final_ref, 7)


def layer(hidden, gain, bias, qkv_rows, out_rows, lengths, positions, keys, values):
    hbm, vmem = pl.BlockSpec(memory_space=pltpu.HBM), pl.BlockSpec(memory_space=pltpu.VMEM)
    dma = pltpu.SemaphoreType.DMA
    return pl.pallas_call(
        layer_kernel,
        name="layer",
        out_shape=(
            jax.ShapeDtypeStruct((6, 8, 8, 2, GROUPS, 4, HD), BF16),
            jax.ShapeDtypeStruct((4, 2 * KVH * HD), BF16),
            jax.ShapeDtypeStruct((8, 4, 512), BF16),
        ),
        in_specs=[hbm] * 9,
        out_specs=(vmem, vmem, vmem),
        scratch_shapes=[
            pltpu.SMEM((4,), jnp.int32),
            pltpu.SMEM((2, 4), jnp.int32),
            pltpu.VMEM((4, 3584), BF16),
            pltpu.VMEM((3584,), BF16),
            pltpu.VMEM((1, 3584), F32),
            pltpu.VMEM((24, HD), BF16),
            pltpu.VMEM((ROWS, 24 * HD), BF16),
            pltpu.VMEM((ROWS, 16 * HD), BF16),
            pltpu.VMEM((40, GROUPS, 4, HD), BF16),
            pltpu.VMEM((8, 512), F32),
            pltpu.VMEM((24, HD), F32),
            pltpu.VMEM((3, 2, 4, HD), F32),
            pltpu.VMEM((4, HERE, KVH * HD), BF16),
            pltpu.VMEM((4, HERE, KVH * HD), BF16),
            pltpu.VMEM((2, 8, 8 * ROWS), BF16),
            pltpu.VMEM((8, 8 * ROWS), BF16),
            pltpu.VMEM((2, 8, 16 * ROWS, HD), BF16),
            pltpu.VMEM((8 * ROWS, 3 * HD), BF16),
            pltpu.VMEM((2, 4, 3 * HD), F32),
            pltpu.VMEM((16, 4, 3 * HD), F32),
            pltpu.VMEM((8, 3, 4, HD), BF16),
            pltpu.VMEM((2, 64, HD), F32),
            pltpu.VMEM((64, HD), F32),
            pltpu.VMEM((64, HERE), F32),
            pltpu.VMEM((64, HERE), BF16),
            pltpu.VMEM((8, 2, 8, HD), F32),
            pltpu.VMEM((8, 2, 8, HD), F32),
            pltpu.VMEM((2, 8, HD), F32),
            pltpu.VMEM((8, 2, 8, HD), F32),
            pltpu.VMEM((8, 4, 512), F32),
            pltpu.VMEM((8, 4, 512), F32),
            pltpu.SemaphoreType.REGULAR, dma((7,)), dma((2, 4)), dma((3,)), dma((3, 8)), dma((3,)), dma((3, 40)), dma((2,)), dma((2,)),
            dma((6,)), dma((16,)), dma((8,)), dma((8,)), dma((8,)), dma((8,)), dma((8,)),
        ],
        compiler_params=pltpu.CompilerParams(
            collective_id=0, has_side_effects=True, vmem_limit_bytes=40 * 2**20
        ),
    )(hidden, gain, bias, qkv_rows, out_rows, lengths, positions, keys, values)


def place_kernel(w_ref, fresh_ref, final_ref, attended_out, fresh_out, qkv_ref, out_ref, attended_ref, sems, small):
    copies = []
    for k in range(6):
        target = out_ref.at[:, k * HD : (k + 1) * HD] if k < 2 else qkv_ref.at[:, (k - 2) * HD : (k - 1) * HD]
        for part in range(PLACE):
            rows = slice(part * 3584 // PLACE, (part + 1) * 3584 // PLACE)
            copies.append(pltpu.make_async_copy(w_ref.at[k, rows], target.at[rows], sems.at[k, part]))
    for copy in copies:
        copy.start()
    copies.append(pltpu.make_async_copy(fresh_ref, fresh_out, small.at[0]))
    copies[-1].start()
    for o in range(8):
        attended_ref[:, o * 448 : (o + 1) * 448] = final_ref[o, :, 0:448]
    copies.append(pltpu.make_async_copy(attended_ref, attended_out, small.at[1]))
    copies[-1].start()
    for copy in copies:
        copy.wait()


def place(w, fresh, final):
    hbm, vmem = pl.BlockSpec(memory_space=pltpu.HBM), pl.BlockSpec(memory_space=pltpu.VMEM)
    return pl.pallas_call(
        place_kernel,
        name="place",
        out_shape=(
            jax.ShapeDtypeStruct((4, 3584), BF16),
            jax.ShapeDtypeStruct((4, 1024), BF16),
            jax.ShapeDtypeStruct((3584, 512), BF16),
            jax.ShapeDtypeStruct((3584, 256), BF16),
        ),
        in_specs=[vmem, vmem, vmem],
        out_specs=(hbm, hbm, hbm, hbm),
        scratch_shapes=[
            pltpu.VMEM((4, 3584), BF16), pltpu.SemaphoreType.DMA((6, PLACE)), pltpu.SemaphoreType.DMA((2,)),
        ],
        compiler_params=pltpu.CompilerParams(vmem_limit_bytes=8 * 2**20),
    )(w, fresh, final)


def body(
    hidden,
    norm_gain,
    qkv_bias,
    qkv_weight,
    out_weight,
    key_cache,
    value_cache,
    cache_len,
    block_pos,
):
    operands = (
        hidden, norm_gain, qkv_bias.reshape(24, HD), qkv_weight, out_weight,
        cache_len, block_pos.T, key_cache, value_cache,
    )
    w, fresh_kv, final = layer(*(pltpu.with_memory_space_constraint(a, pltpu.HBM) for a in operands))
    return place(w.reshape(6, 3584, HD), fresh_kv, final)


def solution(mesh):
    finer = Mesh(
        mesh.devices.reshape(2, 4, 4, 2, mesh.shape["roll"]),
        ("seq_0", "seq_1", "tp_0", "tp_1", "roll"),
    )
    in_specs = (
        P("roll", None),
        P(),
        P(),
        P(SEQ_TP_ROLL, None),
        P(SEQ_TP_ROLL, None),
        P("roll", SEQ_TP, None),
        P("roll", SEQ_TP, None),
        P("roll"),
        P("roll", SEQ_TP),
    )
    out_specs = (P("roll", None), P("roll", None), P(None, TP), P(None, TP))
    return jax.shard_map(body, mesh=finer, in_specs=in_specs, out_specs=out_specs, check_vma=False)
```
